32 devices in a mesh: dp: 2 (over x), cp: 4 (over z), tp: 4 (over y, core).
Axes of the slice: x: 2, y: 2, z: 4, core: 2. Of those that a mesh axis runs over, the one named last changes fastest.
Arguments:
- x: bfloat16 [8192, 2048], P(('dp', 'cp', 'tp')), parts along dimension 0
- idx: int32 [8192, 2], P(('dp', 'cp', 'tp')), parts along dimension 0
- gates: float32 [8192, 2], P(('dp', 'cp', 'tp')), parts along dimension 0
- wq: bfloat16 [2048, 2048], P(None, 'tp')
- wk: bfloat16 [2048, 2048], P(None, 'tp')
- wv: bfloat16 [2048, 2048], P(None, 'tp')
- wo: bfloat16 [2048, 2048], P('tp')
- w1g: bfloat16 [16, 2048, 1024], P(('cp', 'tp'))
- w1u: bfloat16 [16, 2048, 1024], P(('cp', 'tp'))
- w2: bfloat16 [16, 1024, 2048], P(('cp', 'tp'))
Outputs:
- output: bfloat16 [8192, 2048], P(('dp', 'cp', 'tp')), parts along dimension 0
There are 2 independent parts. The reference program is written for one: setup_inputs(seed, part) draws one part's arguments, and reference() takes and returns one part's arrays. A program takes and returns all parts, laid end to end along the dimension named above; an argument that names none is the same for every part.
All inputs are finite; a program needn't handle non-finite values.
Results may differ from the reference program's by a relative error of at most 0.00999393.
Values are sent between devices in bfloat16 or wider.
A program may use at most 1 GiB of HBM per device.

```python
import math
import jax
import jax.numpy as jnp
from jax import lax

H = 2048
FF = 1024
HEADS = 16
KV_HEADS = 16
HEAD = 128
S = 4096
CP = 4
TP = 4
TOP = 2
QBLK = 512

E = CP * TP
T = S // E
CAP = 4 * T // E
M = 2 * T // E


def seg_positions():
    i = jnp.arange(S, dtype=jnp.int32)
    seg = S // (2 * CP)
    b = i // seg
    r = b // 2
    s_id = jnp.where(b % 2 == 0, r, 2 * CP - 1 - r)
    return s_id * seg + i % seg


def source_routing(key, sigma, counts):
    ends = jnp.cumsum(counts)
    labels = sigma[jnp.searchsorted(ends, jnp.arange(2 * T, dtype=jnp.int32), side='right')]
    perm = jax.random.permutation(key, T)
    return jnp.stack([labels[perm], labels[perm + T]], axis=1).astype(jnp.int32)


def setup_inputs(seed: int = 0, part: int = 0) -> dict:
    key = jax.random.key(seed)
    ks = jax.random.split(key, 7)
    kx = jax.random.split(jax.random.fold_in(key, part), 4)
    a = math.log(S / 16.0) ** 0.25

    def nrm(k, shape, scale):
        return (jax.random.normal(k, shape, jnp.float32) * scale).astype(jnp.bfloat16)

    wq = nrm(ks[0], (H, HEADS * HEAD), a / math.sqrt(H))
    wk = nrm(ks[1], (H, KV_HEADS * HEAD), a / math.sqrt(H))
    wv = nrm(ks[2], (H, KV_HEADS * HEAD), 1.0 / math.sqrt(H))
    wo = nrm(ks[3], (HEADS * HEAD, H), 1.0 / math.sqrt(HEADS * HEAD))
    w1g = nrm(ks[4], (E, H, FF), 1.0 / math.sqrt(H))
    w1u = nrm(ks[5], (E, H, FF), 1.0 / math.sqrt(H))
    w2 = nrm(ks[6], (E, FF, H), 1.5 / math.sqrt(FF))
    x = nrm(kx[0], (S, H), 1.0)
    sigmas = jax.vmap(lambda kk: jax.random.permutation(kk, E))(jax.random.split(kx[1], E))
    counts = jnp.full((E,), M, jnp.int32)
    idx = jax.vmap(lambda kk, sg: source_routing(kk, sg, counts))(jax.random.split(kx[2], E), sigmas)
    idx = idx.reshape(S, TOP)
    gates = jax.random.uniform(kx[3], (S, TOP), jnp.float32, 0.3, 0.7)
    return {'x': x, 'idx': idx, 'gates': gates, 'wq': wq, 'wk': wk, 'wv': wv, 'wo': wo, 'w1g': w1g, 'w1u': w1u, 'w2': w2}


def reference(x, idx, gates, wq, wk, wv, wo, w1g, w1u, w2):
    pos = seg_positions()
    g = HEADS // KV_HEADS
    q = jnp.dot(x, wq, preferred_element_type=jnp.float32).astype(jnp.bfloat16)
    k = jnp.dot(x, wk, preferred_element_type=jnp.float32).astype(jnp.bfloat16)
    v = jnp.dot(x, wv, preferred_element_type=jnp.float32).astype(jnp.bfloat16)
    qh = q.reshape(S, HEADS, HEAD).transpose(1, 0, 2)
    kh = jnp.repeat(k.reshape(S, KV_HEADS, HEAD).transpose(1, 0, 2), g, axis=0)
    vh = jnp.repeat(v.reshape(S, KV_HEADS, HEAD).transpose(1, 0, 2), g, axis=0)
    scale = HEAD ** -0.5
    nb = S // QBLK

    def head(args):
        qa, ka, va = args

        def block(bargs):
            qb, pb = bargs
            s = jnp.dot(qb, ka.T, preferred_element_type=jnp.float32) * scale
            mask = pos[None, :] <= pb[:, None]
            s = jnp.where(mask, s, -1e30)
            m = jnp.max(s, axis=-1, keepdims=True)
            w = jnp.where(mask, jnp.exp(s - m), 0.0)
            l = jnp.sum(w, axis=-1, keepdims=True)
            ob = jnp.dot(w.astype(jnp.bfloat16), va, preferred_element_type=jnp.float32)
            return ob / l

        out = lax.map(block, (qa.reshape(nb, QBLK, HEAD), pos.reshape(nb, QBLK)))
        return out.reshape(S, HEAD)

    o = lax.map(head, (qh, kh, vh))
    o = o.transpose(1, 0, 2).reshape(S, HEADS * HEAD).astype(jnp.bfloat16)
    att = jnp.dot(o, wo, preferred_element_type=jnp.float32)
    h = (x.astype(jnp.float32) + att).astype(jnp.bfloat16)

    ea = idx.reshape(-1)
    tok = jnp.arange(S * TOP) // TOP
    onehot = (ea[:, None] == jnp.arange(E)[None, :]).astype(jnp.int32)
    slot = jnp.take_along_axis(jnp.cumsum(onehot, axis=0), ea[:, None], axis=1)[:, 0] - 1
    ct = E * CAP
    buf = jnp.zeros((E, ct, H), jnp.bfloat16).at[ea, slot].set(h[tok])

    def expert(args):
        rows, wg, wu, wd = args
        gg = jnp.dot(rows, wg, preferred_element_type=jnp.float32)
        uu = jnp.dot(rows, wu, preferred_element_type=jnp.float32)
        act = (jax.nn.silu(gg) * uu).astype(jnp.bfloat16)
        return jnp.dot(act, wd, preferred_element_type=jnp.float32).astype(jnp.bfloat16)

    z = lax.map(expert, (buf, w1g, w1u, w2))
    zt = z[ea, slot].astype(jnp.float32).reshape(S, TOP, H)
    y = h.astype(jnp.float32) + jnp.sum(gates[:, :, None] * zt, axis=1)
    return y.astype(jnp.bfloat16)
```

```python
import functools

import jax
import jax.numpy as jnp
from jax import lax
from jax.experimental import pallas as pl
from jax.experimental.pallas import tpu as pltpu
from jax.sharding import PartitionSpec as P

HD = 128
BF = jnp.bfloat16
F32 = jnp.float32
MESH = pl.DeviceIdType.MESH
NEG = -1e30
ANY = pl.BlockSpec(memory_space=pl.ANY)
VM = pl.BlockSpec(memory_space=pltpu.VMEM)
MIB = 2 ** 20


def remote(src, dst, ssem, rsem, c, t):
    return pltpu.make_async_remote_copy(
        src_ref=src, dst_ref=dst, send_sem=ssem, recv_sem=rsem,
        device_id={'cp': c, 'tp': t}, device_id_type=MESH)


def group_barrier(c, t):
    sem = pltpu.get_barrier_semaphore()
    for i in range(1, 16):
        pl.semaphore_signal(sem, inc=1, device_id={'cp': c ^ (i // 4), 'tp': t ^ (i % 4)}, device_id_type=MESH)
    pl.semaphore_wait(sem, 15)


def kernel_a(x_ref, idx_ref, wq_ref, wk_ref, wv_ref, wo_ref,
             qkv_ref, woa_ref, cnt_ref,
             xs, sb, cb, xsend, xrecv, wsend, wrecv, qsend, qrecv, qloc, csend, crecv):
    c = lax.axis_index('cp')
    t = lax.axis_index('tp')
    y = t // 2
    rows = x_ref.shape[0]
    seg = 2 * rows
    nseg = 8
    e = lax.broadcasted_iota(jnp.int32, (rows, HD), 1)
    hit = (idx_ref[:, 0:1] == e).astype(F32) + (idx_ref[:, 1:2] == e).astype(F32)
    load = jnp.max(jnp.sum(hit, axis=0, keepdims=True), axis=1, keepdims=True)
    cb[...] = jnp.broadcast_to(load, cb.shape)
    me = c * 4 + t

    group_barrier(c, t)
    pending = []

    def go(cp):
        cp.start()
        pending.append(cp)

    own = pl.ds(pl.multiple_of(t * rows, rows), rows)
    go(remote(x_ref, xs.at[own], xsend.at[0], xrecv.at[t], c, t ^ 1))
    go(remote(x_ref, xs.at[own], xsend.at[1], xrecv.at[t], c, t ^ 2))
    xs[own, :] = x_ref[...]
    go(remote(wo_ref, woa_ref.at[t], wsend.at[0], wrecv.at[t], c, t ^ 1))
    go(remote(wo_ref, woa_ref.at[t], wsend.at[1], wrecv.at[t], c, t ^ 2))
    for i in range(1, 16):
        go(remote(cb, cnt_ref.at[me], csend.at[i], crecv.at[me], c ^ (i // 4), t ^ (i % 4)))
    cloc = pltpu.make_async_copy(cb, cnt_ref.at[me], csend.at[0])
    cloc.start()

    def xwait(tt):
        r = pl.ds(pl.multiple_of(tt * rows, rows), rows)
        remote(xs.at[r], xs.at[r], xsend.at[0], xrecv.at[tt], c, t ^ 1).wait_recv()

    locs = []

    def half(p, row0, s):
        for m, w in enumerate((wq_ref, wk_ref, wv_ref)):
            r = jnp.dot(xs[pl.ds(row0, seg), :], w[...], preferred_element_type=F32).astype(BF)
            for hh in range(4):
                sb[p, m, hh] = r[:, hh * HD:(hh + 1) * HD]
            dst = qkv_ref.at[m, s]
            for off in (2, 3, 1):
                c2 = c ^ off
                go(remote(sb.at[p, m, c2], dst, qsend.at[p, m, off], qrecv.at[m, s], c2, t))
            lc = pltpu.make_async_copy(sb.at[p, m, c], dst, qloc.at[p, m])
            lc.start()
            locs.append(lc)

    xwait(t ^ 1)
    half(0, pl.multiple_of(y * seg, seg), jnp.where(y == 0, c, nseg - 1 - c))
    xwait(t ^ 2)
    r2 = pl.ds(pl.multiple_of((t ^ 2) * rows, rows), rows)
    go(remote(xs.at[r2], xs.at[r2], xsend.at[2], xrecv.at[t ^ 2], c, t ^ 1))
    xwait(t ^ 3)
    half(1, pl.multiple_of((1 - y) * seg, seg), jnp.where(y == 1, c, nseg - 1 - c))

    def wwait(tt):
        remote(wo_ref, woa_ref.at[tt], wsend.at[0], wrecv.at[tt], c, t ^ 1).wait_recv()

    wwait(t ^ 2)
    go(remote(woa_ref.at[t ^ 2], woa_ref.at[t ^ 2], wsend.at[2], wrecv.at[t ^ 2], c, t ^ 1))
    wwait(t ^ 1)
    wwait(t ^ 3)
    for off in (1, 2, 3):
        c2 = c ^ off
        for s in (c2, nseg - 1 - c2):
            for m in range(3):
                remote(sb.at[0, 0, 0], qkv_ref.at[m, s], qsend.at[0, 0, 0], qrecv.at[m, s], c2, t).wait_recv()
    for i in range(1, 16):
        other = (c ^ (i // 4)) * 4 + (t ^ (i % 4))
        remote(cb, cnt_ref.at[other], csend.at[i], crecv.at[other], c ^ (i // 4), t ^ (i % 4)).wait_recv()
    for cp in pending:
        cp.wait_send()
    for lc in locs:
        lc.wait()
    cloc.wait()


def kernel_b(qkv_ref, x_ref, wo_ref, woa_ref, h_ref,
             qkv, vt, wv, acc, ob, orecv, lsem, wsem, osend, oloc, orsem):
    c = lax.axis_index('cp')
    t = lax.axis_index('tp')
    y = t // 2
    rows = x_ref.shape[0]
    seg = 2 * rows
    nseg = 8
    loads = []
    for m in range(3):
        cp = pltpu.make_async_copy(qkv_ref.at[m], qkv.at[m], lsem.at[m])
        cp.start()
        loads.append(cp)
    wl = []
    for i in range(4):
        tt = t ^ i
        cp = pltpu.make_async_copy(wo_ref if i == 0 else woa_ref.at[tt], wv.at[tt], wsem.at[i])
        cp.start()
        wl.append(cp)
    group_barrier(c, t)
    for cp in loads:
        cp.wait()
    for s in range(nseg):
        vt[:, s * seg:(s + 1) * seg] = qkv[2, s].T
    k2 = (HD ** -0.5) * 1.4426950408889634
    hcol = pl.ds(pl.multiple_of((t * 4 + c) * HD, HD), HD)
    me = c * 4 + t

    def block(s, j, diag, m, l):
        q = qkv[0, s]
        sc = lax.dot_general(qkv[1, j], q, (((1,), (1,)), ((), ())), preferred_element_type=F32)
        if diag:
            ki = lax.broadcasted_iota(jnp.int32, sc.shape, 0)
            qi = lax.broadcasted_iota(jnp.int32, sc.shape, 1)
            sc = jnp.where(ki <= qi, sc, NEG)
        mn = jnp.maximum(m, jnp.max(sc, axis=0, keepdims=True))
        w = jnp.exp2((sc - mn) * k2)
        a = jnp.exp2((m - mn) * k2)
        l = l * a + jnp.sum(w, axis=0, keepdims=True)
        vj = vt[:, pl.ds(pl.multiple_of(j * seg, seg), seg)]
        acc[...] = acc[...] * a + jnp.dot(vj, w.astype(BF), preferred_element_type=F32)
        return mn, l

    def dest(s, hf):
        low = s < 4
        return jnp.where(low, s, nseg - 1 - s), jnp.where(low, hf, 2 + hf)

    def send(s, hf):
        c2, t2 = dest(s, hf)
        src = ob.at[s, pl.ds(hf * rows, rows)]
        rm = remote(src, orecv.at[:, hcol], osend.at[s, hf], orsem.at[me], c2, t2)
        lc = pltpu.make_async_copy(src, orecv.at[:, hcol], oloc.at[0])
        return jnp.logical_and(c2 == c, t2 == t), rm, lc

    def qblock(s, _):
        acc[...] = jnp.zeros_like(acc)
        m = jnp.full((1, seg), NEG, F32)
        l = jnp.zeros((1, seg), F32)
        m, l = lax.fori_loop(0, s, lambda j, ml: block(s, j, False, *ml), (m, l))
        m, l = block(s, s, True, m, l)
        ob[s] = (acc[...] / l).T.astype(BF)
        for hf in range(2):
            mine, rm, lc = send(s, hf)

            @pl.when(jnp.logical_not(mine))
            def _():
                rm.start()

            @pl.when(mine)
            def _():
                lc.start()
        return 0

    lax.fori_loop(0, nseg, qblock, 0)
    for cp in wl:
        cp.wait()
    for i in range(1, 16):
        c2, t2 = c ^ (i // 4), t ^ (i % 4)
        hc = pl.ds(pl.multiple_of((t2 * 4 + c2) * HD, HD), HD)
        remote(ob.at[0, pl.ds(0, rows)], orecv.at[:, hc], osend.at[0, 0], orsem.at[c2 * 4 + t2], c2, t2).wait_recv()
    pltpu.make_async_copy(ob.at[0, pl.ds(0, rows)], orecv.at[:, hcol], oloc.at[0]).wait()
    for nb in range(4):
        cols = slice(nb * 512, (nb + 1) * 512)
        a = x_ref[:, cols].astype(F32)
        p = jnp.zeros_like(a)
        for tt in range(4):
            p = p + jnp.dot(orecv[:, tt * 512:(tt + 1) * 512], wv[tt, :, cols], preferred_element_type=F32)
        h_ref[:, cols] = (a + p).astype(BF)

    def drain(s, _):
        for hf in range(2):
            mine, rm, lc = send(s, hf)

            @pl.when(jnp.logical_not(mine))
            def _():
                rm.wait_send()
        return 0

    lax.fori_loop(0, nseg, drain, 0)


def kernel_c(cap, h_ref, idx_ref, idxt_ref, gates_ref, w1g_ref, w1u_ref, w2_ref, y_ref,
             wg, wu, wd, sb, rb, zb, bb, wsem, dsend, drecv, zsend, zrecv, dloc, zloc):
    c = lax.axis_index('cp')
    t = lax.axis_index('tp')
    me = c * 4 + t
    rows = h_ref.shape[0]
    ne = 16
    wl = [pltpu.make_async_copy(a.at[0], b, wsem.at[i])
          for i, (a, b) in enumerate(((w1g_ref, wg), (w1u_ref, wu), (w2_ref, wd)))]
    for cp in wl:
        cp.start()
    ei = lax.broadcasted_iota(jnp.int32, (HD, rows), 0)
    o0 = (idxt_ref[0:1, :] == ei).astype(F32)
    o1 = (idxt_ref[1:2, :] == ei).astype(F32)
    ri = lax.broadcasted_iota(jnp.int32, (rows, rows), 0)
    ci = lax.broadcasted_iota(jnp.int32, (rows, rows), 1)
    rank = jnp.dot((o0 + o1).astype(BF), (ri < ci).astype(BF), preferred_element_type=F32)
    base = ei.astype(F32) * cap + rank
    d0 = jnp.sum(o0 * base, axis=0, keepdims=True)
    d1 = jnp.sum(o1 * base, axis=0, keepdims=True)
    ki = lax.broadcasted_iota(jnp.int32, (ne * cap, rows), 0).astype(F32)
    pack = jnp.logical_or(ki == d0, ki == d1).astype(BF)
    sb[...] = jnp.dot(pack, h_ref[...], preferred_element_type=F32).astype(BF).reshape(sb.shape)
    group_barrier(c, t)
    order = [(o, i) for o in (2, 3, 1, 0) for i in range(4)]
    sends = []
    for off, i in order:
        c2, t2 = c ^ off, t ^ i
        k2 = c2 * 4 + t2
        if off == 0 and i == 0:
            own = pltpu.make_async_copy(sb.at[me], rb.at[0], dloc.at[0])
            own.start()
        else:
            cp = remote(sb.at[k2], rb.at[off * 4 + i], dsend.at[off * 4 + i], drecv.at[off * 4 + i], c2, t2)
            cp.start()
            sends.append(cp)
    for cp in wl:
        cp.wait()
    for off in (0, 2, 1, 3):
        for i in range(4):
            if off == 0 and i == 0:
                own.wait()
            else:
                remote(sb.at[0], rb.at[off * 4 + i], dsend.at[off * 4 + i], drecv.at[off * 4 + i], c ^ off, t ^ i).wait_recv()
        r = rb[off * 4:off * 4 + 4].reshape(4 * cap, -1)
        g = jnp.dot(r, wg[...], preferred_element_type=F32)
        u = jnp.dot(r, wu[...], preferred_element_type=F32)
        a = (g * jax.nn.sigmoid(g) * u).astype(BF)
        z = jnp.dot(a, wd[...], preferred_element_type=F32).astype(BF)
        zb[off * 4:off * 4 + 4] = z.reshape(4, cap, -1)
        for i in range(4):
            k = off * 4 + i
            if k == 0:
                zown = pltpu.make_async_copy(zb.at[0], bb.at[me], zloc.at[0])
                zown.start()
            else:
                cp = remote(zb.at[k], bb.at[me], zsend.at[k], zrecv.at[k], c ^ off, t ^ i)
                cp.start()
                sends.append(cp)
    ej = lax.broadcasted_iota(jnp.int32, (rows, HD), 1)
    q0 = (idx_ref[:, 0:1] == ej).astype(F32)
    q1 = (idx_ref[:, 1:2] == ej).astype(F32)
    rk = jnp.dot((ci < ri).astype(BF), (q0 + q1).astype(BF), preferred_element_type=F32)
    bs = ej.astype(F32) * cap + rk
    f0 = jnp.sum(q0 * bs, axis=1, keepdims=True)
    f1 = jnp.sum(q1 * bs, axis=1, keepdims=True)
    kj = lax.broadcasted_iota(jnp.int32, (rows, ne * cap), 1).astype(F32)
    s0 = (kj == f0).astype(BF)
    s1 = (kj == f1).astype(BF)
    zown.wait()
    for k in range(1, 16):
        c2, t2 = c ^ (k // 4), t ^ (k % 4)
        remote(zb.at[0], bb.at[c2 * 4 + t2], zsend.at[k], zrecv.at[k], c2, t2).wait_recv()
    for nb in range(4):
        cols = slice(nb * 512, (nb + 1) * 512)
        b = bb[:, :, cols].reshape(ne * cap, 512)
        z0 = jnp.dot(s0, b, preferred_element_type=F32)
        z1 = jnp.dot(s1, b, preferred_element_type=F32)
        acc = gates_ref[:, 0:1] * z0 + gates_ref[:, 1:2] * z1
        y_ref[:, cols] = (h_ref[:, cols].astype(F32) + acc).astype(BF)
    for cp in sends:
        cp.wait_send()


def params(cid):
    return pltpu.CompilerParams(collective_id=cid, has_side_effects=True, vmem_limit_bytes=60 * MIB)


def solution(mesh):
    rows_spec = P(('dp', 'cp', 'tp'), None)
    exp_spec = P(('cp', 'tp'), None, None)
    DMA = pltpu.SemaphoreType.DMA

    def local(x, idx, gates, wq, wk, wv, wo, w1g, w1u, w2):
        rows, d = x.shape
        seg = 2 * rows
        hc = wq.shape[1]
        ff = w1g.shape[2]
        sds = jax.ShapeDtypeStruct
        qkv, woa, cnt = pl.pallas_call(
            kernel_a, name='qkv_exchange',
            out_shape=(sds((3, 8, seg, HD), BF), sds((4, hc, d), BF), sds((16, 8, HD), F32)),
            in_specs=[VM, VM, VM, VM, VM, ANY], out_specs=(ANY, ANY, ANY),
            scratch_shapes=[
                pltpu.VMEM((4 * rows, d), BF), pltpu.VMEM((2, 3, 4, seg, HD), BF), pltpu.VMEM((8, HD), F32),
                DMA((3,)), DMA((4,)), DMA((3,)), DMA((4,)), DMA((2, 3, 4)), DMA((3, 8)), DMA((2, 3)), DMA((16,)), DMA((16,))],
            compiler_params=params(0))(x, idx, wq, wk, wv, wo)
        h = pl.pallas_call(
            kernel_b, name='attention',
            out_shape=sds((rows, d), BF),
            in_specs=[ANY, VM, ANY, ANY], out_specs=VM,
            scratch_shapes=[
                pltpu.VMEM((3, 8, seg, HD), BF), pltpu.VMEM((HD, 8 * seg), BF), pltpu.VMEM((4, hc, d), BF),
                pltpu.VMEM((HD, seg), F32), pltpu.VMEM((8, seg, HD), BF), pltpu.VMEM((rows, d), BF),
                DMA((3,)), DMA((4,)), DMA((8, 2)), DMA((1,)), DMA((16,))],
            compiler_params=params(1))(qkv, x, wo, woa)
        worst = jnp.max(cnt)

        def experts(cap, cid):
            def f(h, idx, idxt, gates, w1g, w1u, w2):
                return pl.pallas_call(
                    functools.partial(kernel_c, cap), name=f'experts{cap}',
                    out_shape=sds((rows, d), BF),
                    in_specs=[VM, VM, VM, VM, ANY, ANY, ANY], out_specs=VM,
                    scratch_shapes=[
                        pltpu.VMEM((d, ff), BF), pltpu.VMEM((d, ff), BF), pltpu.VMEM((ff, d), BF),
                        pltpu.VMEM((16, cap, d), BF), pltpu.VMEM((16, cap, d), BF), pltpu.VMEM((16, cap, d), BF), pltpu.VMEM((16, cap, d), BF),
                        DMA((3,)), DMA((16,)), DMA((16,)), DMA((16,)), DMA((16,)), DMA((1,)), DMA((1,))],
                    compiler_params=params(cid))(h, idx, idxt, gates, w1g, w1u, w2)
            return f

        caps = (32, 48, 64)
        which = (worst > caps[0]).astype(jnp.int32) + (worst > caps[1]).astype(jnp.int32)
        return lax.switch(which, [experts(cp, 2 + i) for i, cp in enumerate(caps)], h, idx, idx.T, gates, w1g, w1u, w2)

    return jax.shard_map(local, mesh=mesh, in_specs=(rows_spec, rows_spec, rows_spec, P(None, 'tp'), P(None, 'tp'), P(None, 'tp'), P('tp', None), exp_spec, exp_spec, exp_spec), out_specs=rows_spec, check_vma=False)
```

```python
import functools

import jax
import jax.numpy as jnp
from jax import lax
from jax.experimental import pallas as pl
from jax.experimental.pallas import tpu as pltpu
from jax.sharding import PartitionSpec as P

HD = 128
BF = jnp.bfloat16
F32 = jnp.float32
MESH = pl.DeviceIdType.MESH
NEG = -1e30
ANY = pl.BlockSpec(memory_space=pl.ANY)
VM = pl.BlockSpec(memory_space=pltpu.VMEM)
MIB = 2 ** 20
CAPS = (32, 48, 64)


def remote(src, dst, ssem, rsem, c, t):
    return pltpu.make_async_remote_copy(
        src_ref=src, dst_ref=dst, send_sem=ssem, recv_sem=rsem,
        device_id={'cp': c, 'tp': t}, device_id_type=MESH)


def group_barrier(c, t):
    sem = pltpu.get_barrier_semaphore()
    for i in range(1, 16):
        pl.semaphore_signal(sem, inc=1, device_id={'cp': c ^ (i // 4), 'tp': t ^ (i % 4)}, device_id_type=MESH)
    pl.semaphore_wait(sem, 15)


def kernel_ab(x_ref, idx_ref, wq_ref, wk_ref, wv_ref, wo_ref, h_ref, which_ref,
              xs, wq, wk, wv, sqk, sv, qk, vt, acc, mx, ls, wob, ob, orecv, cb, cnt,
              ldsem, xsend, xrecv, wsend, wrecv, bsend, brecv, bloc, osend, orsem, csend, crecv):
    c = lax.axis_index('cp')
    t = lax.axis_index('tp')
    y = t // 2
    odd = lax.rem(t, 2) == 1
    rows = idx_ref.shape[0]
    seg = 2 * rows
    nseg = 8
    me = c * 4 + t

    def has(cc, sl, s):
        outer = jnp.logical_or(s < 2, s > 5)
        kvg = jnp.where(cc < 2, outer, jnp.logical_not(outer))
        if sl == 0:
            return kvg
        return jnp.where(odd, jnp.where(cc < 2, s < 2, s >= 2), kvg)

    def sees(cc, sl, s):
        top = jnp.where(cc < 2, 7, 5)
        if sl == 1:
            top = jnp.where(odd, jnp.where(cc < 2, 1, 7), top)
        return s <= top

    own = pl.ds(pl.multiple_of(t * rows, rows), rows)
    loads = [pltpu.make_async_copy(a, b, ldsem.at[i])
             for i, (a, b) in enumerate(((x_ref, xs.at[own]), (wk_ref, wk), (wv_ref, wv), (wq_ref, wq), (wo_ref, wob.at[t])))]
    for cp in loads:
        cp.start()
    e = lax.broadcasted_iota(jnp.int32, (rows, HD), 1)
    hit = (idx_ref[:, 0:1] == e).astype(F32) + (idx_ref[:, 1:2] == e).astype(F32)
    load = jnp.max(jnp.sum(hit, axis=0, keepdims=True), axis=1, keepdims=True)
    cb[...] = jnp.broadcast_to(load, cb.shape)
    cnt[me] = cb[...]
    group_barrier(c, t)
    pending = []

    def go(cp):
        cp.start()
        pending.append(cp)

    loads[0].wait()
    go(remote(xs.at[own], xs.at[own], xsend.at[0], xrecv.at[t], c, t ^ 1))
    go(remote(xs.at[own], xs.at[own], xsend.at[1], xrecv.at[t], c, t ^ 2))

    def xwait(tt):
        r = pl.ds(pl.multiple_of(tt * rows, rows), rows)
        remote(xs.at[r], xs.at[r], xsend.at[0], xrecv.at[tt], c, t ^ 1).wait_recv()

    def blocks(m, p, cc, sl, s):
        hd = 2 * sl + lax.rem(cc, 2)
        if m == 2:
            return sv.at[p, hd], vt.at[sl, s]
        return sqk.at[p, m, hd], qk.at[sl, m, s]

    def need(m, cc, sl, s):
        return has(cc, sl, s) if m == 0 else sees(cc, sl, s)

    def block_copy(m, p, off, sl, s):
        cc = c ^ off
        src, dst = blocks(m, p, cc, sl, s)
        return need(m, cc, sl, s), remote(src, dst, bsend.at[p, m, off, sl], brecv.at[sl, m, s], cc, t)

    def own_copy(m, p, sl, s):
        src, dst = blocks(m, p, c, sl, s)
        return need(m, c, sl, s), pltpu.make_async_copy(src, dst, bloc.at[p, m, sl])

    def half(p, row0, s):
        for m, w, ld in ((1, wk, 1), (2, wv, 2), (0, wq, 3)):
            if p == 0:
                loads[ld].wait()
            r = jnp.dot(xs[pl.ds(row0, seg), :], w[...], preferred_element_type=F32)
            if m == 2:
                rt = r.T.astype(BF)
                for hh in range(4):
                    sv[p, hh] = rt[hh * HD:(hh + 1) * HD]
            else:
                r = r.astype(BF)
                for hh in range(4):
                    sqk[p, m, hh] = r[:, hh * HD:(hh + 1) * HD]
            for off in (1, 2, 3):
                for sl in range(2):
                    ok, cp = block_copy(m, p, off, sl, s)
                    pl.when(ok)(cp.start)
            for sl in range(2):
                ok, cp = own_copy(m, p, sl, s)
                pl.when(ok)(cp.start)

    seg0 = jnp.where(y == 0, c, nseg - 1 - c)
    seg1 = jnp.where(y == 0, nseg - 1 - c, c)
    xwait(t ^ 1)
    half(0, pl.multiple_of(y * seg, seg), seg0)
    loads[4].wait()
    go(remote(wob.at[t], wob.at[t], wsend.at[0], wrecv.at[t], c, t ^ 1))
    go(remote(wob.at[t], wob.at[t], wsend.at[1], wrecv.at[t], c, t ^ 2))
    for i in range(1, 16):
        go(remote(cb, cnt.at[me], csend.at[i], crecv.at[me], c ^ (i // 4), t ^ (i % 4)))
    acc[...] = jnp.zeros_like(acc)
    mx[...] = jnp.full_like(mx, NEG)
    ls[...] = jnp.zeros_like(ls)
    xwait(t ^ 2)
    r2 = pl.ds(pl.multiple_of((t ^ 2) * rows, rows), rows)
    go(remote(xs.at[r2], xs.at[r2], xsend.at[2], xrecv.at[t ^ 2], c, t ^ 1))
    xwait(t ^ 3)
    half(1, pl.multiple_of((1 - y) * seg, seg), seg1)

    k2 = (HD ** -0.5) * 1.4426950408889634

    def unit(sl, q, j, diag):
        sc = lax.dot_general(qk[sl, 1, j], qk[sl, 0, q], (((1,), (1,)), ((), ())), preferred_element_type=F32)
        if diag:
            ki = lax.broadcasted_iota(jnp.int32, sc.shape, 0)
            qi = lax.broadcasted_iota(jnp.int32, sc.shape, 1)
            sc = jnp.where(ki <= qi, sc, NEG)
        m = mx[sl, q]
        mn = jnp.maximum(m, jnp.max(sc, axis=0, keepdims=True))
        w = jnp.exp2((sc - mn) * k2)
        a = jnp.exp2((m - mn) * k2)
        mx[sl, q] = mn
        ls[sl, q] = ls[sl, q] * a + jnp.sum(w, axis=0, keepdims=True)
        acc[sl, q] = acc[sl, q] * a + jnp.dot(vt[sl, j], w.astype(BF), preferred_element_type=F32)

    inner = jnp.logical_or(c == 1, c == 2)

    def off_of(i):
        r = lax.rem(i, 4)
        far = jnp.where(inner, 5 - r, r)
        return jnp.where(r < 2, r, far)

    def seg_of(i):
        cc = c ^ off_of(i)
        low = (i < 4) == (y == 0)
        return jnp.where(low, cc, nseg - 1 - cc)

    def pos_of(s):
        low = s < 4
        off = jnp.where(low, s, nseg - 1 - s) ^ c
        far = jnp.where(inner, 5 - off, off)
        return jnp.where(low == (y == 0), 0, 4) + jnp.where(off < 2, off, far)

    def dest(s, hf):
        low = s < 4
        return jnp.where(low, s, nseg - 1 - s), jnp.where(low, hf, 2 + hf)

    def ocopy(sl, s, hf):
        c2, t2 = dest(s, hf)
        hd = t * 4 + 2 * sl + lax.rem(c, 2)
        src = ob.at[sl, s, pl.ds(hf * rows, rows)]
        dst = orecv.at[:, pl.ds(pl.multiple_of(hd * HD, HD), HD)]
        rm = remote(src, dst, osend.at[sl, s, hf], orsem.at[hd], c2, t2)
        lc = pltpu.make_async_copy(src, dst, orsem.at[hd])
        return jnp.logical_and(c2 == c, t2 == t), rm, lc

    def finish(sl, s):
        ob[sl, s] = (acc[sl, s] / ls[sl, s]).T.astype(BF)
        for hf in range(2):
            mine, rm, lc = ocopy(sl, s, hf)
            pl.when(jnp.logical_not(mine))(rm.start)
            pl.when(mine)(lc.start)

    def event(i, _):
        s = seg_of(i)
        off = off_of(i)
        p = i // 4
        for sl in range(2):
            for m in range(3):
                src, dst = blocks(m, 0, c, sl, s)
                lsrc, _d = blocks(m, p, c, sl, s)
                pl.when(jnp.logical_and(need(m, c, sl, s), off != 0))(
                    remote(src, dst, bsend.at[0, 0, 0, 0], brecv.at[sl, m, s], c, t ^ 1).wait_recv)
                pl.when(jnp.logical_and(need(m, c, sl, s), off == 0))(
                    pltpu.make_async_copy(lsrc, dst, bloc.at[p, m, sl]).wait)

        def pair(k, _):
            s2 = seg_of(k)
            q, j = jnp.maximum(s, s2), jnp.minimum(s, s2)
            for sl in range(2):
                @pl.when(has(c, sl, q))
                def _():
                    unit(sl, q, j, False)
            return 0

        lax.fori_loop(0, i, pair, 0)
        for sl in range(2):
            @pl.when(has(c, sl, s))
            def _():
                unit(sl, s, s, True)

        def done(q, last):
            last = jnp.maximum(last, pos_of(q))
            for sl in range(2):
                @pl.when(jnp.logical_and(last == i, has(c, sl, q)))
                def _():
                    finish(sl, q)
            return last

        lax.fori_loop(0, nseg, done, 0)
        return 0

    lax.fori_loop(0, 2 * 4, event, 0)

    def wwait(tt):
        remote(wob.at[t], wob.at[tt], wsend.at[0], wrecv.at[tt], c, t ^ 1).wait_recv()

    wwait(t ^ 2)
    go(remote(wob.at[t ^ 2], wob.at[t ^ 2], wsend.at[2], wrecv.at[t ^ 2], c, t ^ 1))
    for i in range(1, 16):
        other = (c ^ (i // 4)) * 4 + (t ^ (i % 4))
        remote(cb, cnt.at[other], csend.at[i], crecv.at[other], c ^ (i // 4), t ^ (i % 4)).wait_recv()
    worst = jnp.max(cnt[...])
    which_ref[0] = (worst > CAPS[0]).astype(jnp.int32) + (worst > CAPS[1]).astype(jnp.int32)
    for tt in range(4):
        for hd in range(4):
            k = tt * 4 + hd
            half_b = jnp.logical_and(seg0 >= 2, seg0 <= 5)
            if hd >= 2 and tt % 2 == 1:
                half_b = seg0 >= 2
            cp_ = jnp.where(half_b, 2, 0) + hd % 2
            mine = jnp.logical_and(cp_ == c, t == tt)
            dst = orecv.at[:, k * HD:(k + 1) * HD]
            src = ob.at[0, 0, pl.ds(0, rows)]
            pl.when(jnp.logical_not(mine))(remote(src, dst, osend.at[0, 0, 0], orsem.at[k], c, t ^ 1).wait_recv)
            pl.when(mine)(pltpu.make_async_copy(src, dst, orsem.at[k]).wait)
    wwait(t ^ 1)
    wwait(t ^ 3)
    for nb in range(4):
        cols = slice(nb * 512, (nb + 1) * 512)
        a = xs[own, cols].astype(F32)
        p = jnp.zeros_like(a)
        for tt in range(4):
            p = p + jnp.dot(orecv[:, tt * 512:(tt + 1) * 512], wob[tt, :, cols], preferred_element_type=F32)
        h_ref[:, cols] = (a + p).astype(BF)
    for cp in pending:
        cp.wait_send()
    for p, s in ((0, seg0), (1, seg1)):
        for m in range(3):
            for off in (1, 2, 3):
                for sl in range(2):
                    ok, cp = block_copy(m, p, off, sl, s)
                    pl.when(ok)(cp.wait_send)

    def drain(s, _):
        for sl in range(2):
            for hf in range(2):
                mine, rm, lc = ocopy(sl, s, hf)
                pl.when(jnp.logical_and(has(c, sl, s), jnp.logical_not(mine)))(rm.wait_send)
        return 0

    lax.fori_loop(0, nseg, drain, 0)


def kernel_c(cap, h_ref, idx_ref, idxt_ref, gates_ref, w1g_ref, w1u_ref, w2_ref, y_ref,
             wg, wu, wd, sb, rb, zb, bb, wsem, dsend, drecv, zsend, zrecv, dloc, zloc):
    c = lax.axis_index('cp')
    t = lax.axis_index('tp')
    me = c * 4 + t
    rows = h_ref.shape[0]
    ne = 16
    wl = [pltpu.make_async_copy(a.at[0], b, wsem.at[i])
          for i, (a, b) in enumerate(((w1g_ref, wg), (w1u_ref, wu), (w2_ref, wd)))]
    for cp in wl:
        cp.start()
    ei = lax.broadcasted_iota(jnp.int32, (HD, rows), 0)
    o0 = (idxt_ref[0:1, :] == ei).astype(F32)
    o1 = (idxt_ref[1:2, :] == ei).astype(F32)
    ri = lax.broadcasted_iota(jnp.int32, (rows, rows), 0)
    ci = lax.broadcasted_iota(jnp.int32, (rows, rows), 1)
    rank = jnp.dot((o0 + o1).astype(BF), (ri < ci).astype(BF), preferred_element_type=F32)
    base = ei.astype(F32) * cap + rank
    d0 = jnp.sum(o0 * base, axis=0, keepdims=True)
    d1 = jnp.sum(o1 * base, axis=0, keepdims=True)
    ki = lax.broadcasted_iota(jnp.int32, (ne * cap, rows), 0).astype(F32)
    pack = jnp.logical_or(ki == d0, ki == d1).astype(BF)
    sb[...] = jnp.dot(pack, h_ref[...], preferred_element_type=F32).astype(BF).reshape(sb.shape)
    group_barrier(c, t)
    order = [(o, i) for o in (1, 2, 3, 0) for i in range(4)]
    sends = []
    for off, i in order:
        c2, t2 = c ^ off, t ^ i
        k2 = c2 * 4 + t2
        if off == 0 and i == 0:
            own = pltpu.make_async_copy(sb.at[me], rb.at[0], dloc.at[0])
            own.start()
        else:
            cp = remote(sb.at[k2], rb.at[off * 4 + i], dsend.at[off * 4 + i], drecv.at[off * 4 + i], c2, t2)
            cp.start()
            sends.append(cp)
    for cp in wl:
        cp.wait()
    for off in (0, 2, 1, 3):
        for i in range(4):
            if off == 0 and i == 0:
                own.wait()
            else:
                remote(sb.at[0], rb.at[off * 4 + i], dsend.at[off * 4 + i], drecv.at[off * 4 + i], c ^ off, t ^ i).wait_recv()
        r = rb[off * 4:off * 4 + 4].reshape(4 * cap, -1)
        g = jnp.dot(r, wg[...], preferred_element_type=F32)
        u = jnp.dot(r, wu[...], preferred_element_type=F32)
        a = (g * jax.nn.sigmoid(g) * u).astype(BF)
        z = jnp.dot(a, wd[...], preferred_element_type=F32).astype(BF)
        zb[off * 4:off * 4 + 4] = z.reshape(4, cap, -1)
        for i in range(4):
            k = off * 4 + i
            if k == 0:
                zown = pltpu.make_async_copy(zb.at[0], bb.at[me], zloc.at[0])
                zown.start()
            else:
                cp = remote(zb.at[k], bb.at[me], zsend.at[k], zrecv.at[k], c ^ off, t ^ i)
                cp.start()
                sends.append(cp)
    ej = lax.broadcasted_iota(jnp.int32, (rows, HD), 1)
    q0 = (idx_ref[:, 0:1] == ej).astype(F32)
    q1 = (idx_ref[:, 1:2] == ej).astype(F32)
    rk = jnp.dot((ci < ri).astype(BF), (q0 + q1).astype(BF), preferred_element_type=F32)
    bs = ej.astype(F32) * cap + rk
    f0 = jnp.sum(q0 * bs, axis=1, keepdims=True)
    f1 = jnp.sum(q1 * bs, axis=1, keepdims=True)
    kj = lax.broadcasted_iota(jnp.int32, (rows, ne * cap), 1).astype(F32)
    s0 = (kj == f0).astype(BF)
    s1 = (kj == f1).astype(BF)
    zown.wait()
    for k in range(1, 16):
        c2, t2 = c ^ (k // 4), t ^ (k % 4)
        remote(zb.at[0], bb.at[c2 * 4 + t2], zsend.at[k], zrecv.at[k], c2, t2).wait_recv()
    for nb in range(4):
        cols = slice(nb * 512, (nb + 1) * 512)
        b = bb[:, :, cols].reshape(ne * cap, 512)
        z0 = jnp.dot(s0, b, preferred_element_type=F32)
        z1 = jnp.dot(s1, b, preferred_element_type=F32)
        acc = gates_ref[:, 0:1] * z0 + gates_ref[:, 1:2] * z1
        y_ref[:, cols] = (h_ref[:, cols].astype(F32) + acc).astype(BF)
    for cp in sends:
        cp.wait_send()


def params(cid):
    return pltpu.CompilerParams(collective_id=cid, has_side_effects=True, vmem_limit_bytes=60 * MIB)


def solution(mesh):
    rows_spec = P(('dp', 'cp', 'tp'), None)
    exp_spec = P(('cp', 'tp'), None, None)
    DMA = pltpu.SemaphoreType.DMA

    def local(x, idx, gates, wq, wk, wv, wo, w1g, w1u, w2):
        rows, d = x.shape
        seg = 2 * rows
        hc = wq.shape[1]
        ff = w1g.shape[2]
        sds = jax.ShapeDtypeStruct
        h, which = pl.pallas_call(
            kernel_ab, name='attention',
            out_shape=(sds((rows, d), BF), sds((1,), jnp.int32)),
            in_specs=[ANY, VM, ANY, ANY, ANY, ANY], out_specs=(VM, pl.BlockSpec(memory_space=pltpu.SMEM)),
            scratch_shapes=[
                pltpu.VMEM((4 * rows, d), BF), pltpu.VMEM((d, hc), BF), pltpu.VMEM((d, hc), BF), pltpu.VMEM((d, hc), BF),
                pltpu.VMEM((2, 2, 4, seg, HD), BF), pltpu.VMEM((2, 4, HD, seg), BF),
                pltpu.VMEM((2, 2, 8, seg, HD), BF), pltpu.VMEM((2, 8, HD, seg), BF),
                pltpu.VMEM((2, 8, HD, seg), F32), pltpu.VMEM((2, 8, 1, seg), F32), pltpu.VMEM((2, 8, 1, seg), F32),
                pltpu.VMEM((4, hc, d), BF), pltpu.VMEM((2, 8, seg, HD), BF), pltpu.VMEM((rows, d), BF),
                pltpu.VMEM((8, HD), F32), pltpu.VMEM((16, 8, HD), F32),
                DMA((5,)), DMA((3,)), DMA((4,)), DMA((3,)), DMA((4,)), DMA((2, 3, 4, 2)), DMA((2, 3, 8)), DMA((2, 3, 2)),
                DMA((2, 8, 2)), DMA((16,)), DMA((16,)), DMA((16,))],
            compiler_params=params(0))(x, idx, wq, wk, wv, wo)

        def experts(cap, cid):
            def f(h, idx, idxt, gates, w1g, w1u, w2):
                return pl.pallas_call(
                    functools.partial(kernel_c, cap), name=f'experts{cap}',
                    out_shape=sds((rows, d), BF),
                    in_specs=[VM, VM, VM, VM, ANY, ANY, ANY], out_specs=VM,
                    scratch_shapes=[
                        pltpu.VMEM((d, ff), BF), pltpu.VMEM((d, ff), BF), pltpu.VMEM((ff, d), BF),
                        pltpu.VMEM((16, cap, d), BF), pltpu.VMEM((16, cap, d), BF), pltpu.VMEM((16, cap, d), BF), pltpu.VMEM((16, cap, d), BF),
                        DMA((3,)), DMA((16,)), DMA((16,)), DMA((16,)), DMA((16,)), DMA((1,)), DMA((1,))],
                    compiler_params=params(cid))(h, idx, idxt, gates, w1g, w1u, w2)
            return f

        return lax.switch(which[0], [experts(cp, 1 + i) for i, cp in enumerate(CAPS)], h, idx, idx.T, gates, w1g, w1u, w2)

    return jax.shard_map(local, mesh=mesh, in_specs=(rows_spec, rows_spec, rows_spec, P(None, 'tp'), P(None, 'tp'), P(None, 'tp'), P('tp', None), exp_spec, exp_spec, exp_spec), out_specs=rows_spec, check_vma=False)
```

```python
import functools

import jax
import jax.numpy as jnp
from jax import lax
from jax.experimental import pallas as pl
from jax.experimental.pallas import tpu as pltpu
from jax.sharding import PartitionSpec as P

HD = 128
BF = jnp.bfloat16
F32 = jnp.float32
MESH = pl.DeviceIdType.MESH
NEG = -1e30
ANY = pl.BlockSpec(memory_space=pl.ANY)
VM = pl.BlockSpec(memory_space=pltpu.VMEM)
MIB = 2 ** 20
BASE_CAP, FULL_CAP = 32, 64
ORDER = (4, 5, 6, 7, 8, 9, 10, 11, 12, 13, 14, 15, 1, 2, 3, 0)


def remote(src, dst, ssem, rsem, c, t):
    return pltpu.make_async_remote_copy(
        src_ref=src, dst_ref=dst, send_sem=ssem, recv_sem=rsem,
        device_id={'cp': c, 'tp': t}, device_id_type=MESH)


def group_barrier(c, t):
    sem = pltpu.get_barrier_semaphore()
    for i in range(1, 16):
        pl.semaphore_signal(sem, inc=1, device_id={'cp': c ^ (i // 4), 'tp': t ^ (i % 4)}, device_id_type=MESH)
    pl.semaphore_wait(sem, 15)


def kernel_ab(x_ref, it_ref, gt_ref, wq_ref, wk_ref, wv_ref, wo_ref, w1g_ref, w1u_ref, w2_ref,
              y_ref, h_out, over_ref,
              xs, wq, wk, wv, sqk, sv, qk, vt, acc, mx, ls, wob, ob, orecv, hs, cb, cnt,
              wg, wu, wd, sb, rb, zb, bb,
              ldsem, xsend, xrecv, wsend, wrecv, bsend, brecv, bloc, osend, orsem, csend, crecv, hsem, esem, *csems):
    c = lax.axis_index('cp')
    t = lax.axis_index('tp')
    y = t // 2
    odd = lax.rem(t, 2) == 1
    rows = it_ref.shape[1]
    seg = 2 * rows
    nseg = 8
    me = c * 4 + t

    def has(cc, sl, s):
        outer = jnp.logical_or(s < 2, s > 5)
        kvg = jnp.where(cc < 2, outer, jnp.logical_not(outer))
        moved = jnp.where(cc < 2, s < 2, s >= 2)
        return jnp.where(jnp.logical_and(odd, sl == 1), moved, kvg)

    def sees(cc, sl, s):
        moved = jnp.where(cc < 2, 1, 7)
        return s <= jnp.where(jnp.logical_and(odd, sl == 1), moved, jnp.where(cc < 2, 7, 5))

    own = pl.ds(pl.multiple_of(t * rows, rows), rows)
    loads = [pltpu.make_async_copy(a, b, ldsem.at[i])
             for i, (a, b) in enumerate(((x_ref, xs.at[own]), (wk_ref, wk), (wv_ref, wv), (wq_ref, wq), (wo_ref, wob.at[t])))]
    for cp in loads:
        cp.start()
    e = lax.broadcasted_iota(jnp.int32, (HD, rows), 0)
    hit = (it_ref[0:1, :] == e).astype(F32) + (it_ref[1:2, :] == e).astype(F32)
    load = jnp.max(jnp.sum(hit, axis=1, keepdims=True), axis=0, keepdims=True)
    cb[...] = jnp.broadcast_to(load, cb.shape)
    cnt[me] = cb[...]
    group_barrier(c, t)
    pending = []

    def go(cp):
        cp.start()
        pending.append(cp)

    loads[0].wait()
    go(remote(xs.at[own], xs.at[own], xsend.at[0], xrecv.at[t], c, t ^ 1))
    go(remote(xs.at[own], xs.at[own], xsend.at[1], xrecv.at[t], c, t ^ 2))

    def xwait(tt):
        r = pl.ds(pl.multiple_of(tt * rows, rows), rows)
        remote(xs.at[r], xs.at[r], xsend.at[0], xrecv.at[tt], c, t ^ 1).wait_recv()

    def blocks(m, p, cc, sl, s):
        hd = 2 * sl + lax.rem(cc, 2)
        if m == 2:
            return sv.at[p, hd], vt.at[sl, s]
        return sqk.at[p, m, hd], qk.at[sl, m, s]

    def need(m, cc, sl, s):
        return has(cc, sl, s) if m == 0 else sees(cc, sl, s)

    def block_copy(m, p, off, sl, s):
        cc = c ^ off
        src, dst = blocks(m, p, cc, sl, s)
        return need(m, cc, sl, s), remote(src, dst, bsend.at[p, m, off, sl], brecv.at[sl, m, s], cc, t)

    def own_copy(m, p, sl, s):
        src, dst = blocks(m, p, c, sl, s)
        return need(m, c, sl, s), pltpu.make_async_copy(src, dst, bloc.at[p, m, sl])

    def half(p, row0, s):
        for sl in range(2):
            wide = slice(2 * sl * HD, 2 * (sl + 1) * HD)
            for m, w, ld in ((1, wk, 1), (2, wv, 2), (0, wq, 3)):
                if p == 0 and sl == 0:
                    loads[ld].wait()
                r = jnp.dot(xs[pl.ds(row0, seg), :], w[:, wide], preferred_element_type=F32)
                if m == 2:
                    rt = r.T.astype(BF)
                    for hh in range(2):
                        sv[p, 2 * sl + hh] = rt[hh * HD:(hh + 1) * HD]
                else:
                    r = r.astype(BF)
                    for hh in range(2):
                        sqk[p, m, 2 * sl + hh] = r[:, hh * HD:(hh + 1) * HD]
                for off in (1, 2, 3):
                    ok, cp = block_copy(m, p, off, sl, s)
                    pl.when(ok)(cp.start)
                ok, cp = own_copy(m, p, sl, s)
                pl.when(ok)(cp.start)

    seg0 = jnp.where(y == 0, c, nseg - 1 - c)
    seg1 = jnp.where(y == 0, nseg - 1 - c, c)
    xwait(t ^ 1)
    half(0, pl.multiple_of(y * seg, seg), seg0)
    loads[4].wait()
    go(remote(wob.at[t], wob.at[t], wsend.at[0], wrecv.at[t], c, t ^ 1))
    go(remote(wob.at[t], wob.at[t], wsend.at[1], wrecv.at[t], c, t ^ 2))
    for i in range(1, 16):
        go(remote(cb, cnt.at[me], csend.at[i], crecv.at[me], c ^ (i // 4), t ^ (i % 4)))
    acc[...] = jnp.zeros_like(acc)
    mx[...] = jnp.full_like(mx, NEG)
    ls[...] = jnp.zeros_like(ls)
    xwait(t ^ 2)
    r2 = pl.ds(pl.multiple_of((t ^ 2) * rows, rows), rows)
    go(remote(xs.at[r2], xs.at[r2], xsend.at[2], xrecv.at[t ^ 2], c, t ^ 1))
    xwait(t ^ 3)
    half(1, pl.multiple_of((1 - y) * seg, seg), seg1)
    wl = expert_loads(w1g_ref, w1u_ref, w2_ref, wg, wu, wd, esem)
    for cp in wl:
        cp.start()

    k2 = (HD ** -0.5) * 1.4426950408889634

    def unit(sl, q, j, diag):
        sc = lax.dot_general(qk[sl, 1, j], qk[sl, 0, q], (((1,), (1,)), ((), ())), preferred_element_type=F32)
        if diag:
            ki = lax.broadcasted_iota(jnp.int32, sc.shape, 0)
            qi = lax.broadcasted_iota(jnp.int32, sc.shape, 1)
            sc = jnp.where(ki <= qi, sc, NEG)
        m = mx[sl, q]
        mn = jnp.maximum(m, jnp.max(sc, axis=0, keepdims=True))
        w = jnp.exp2((sc - mn) * k2)
        a = jnp.exp2((m - mn) * k2)
        mx[sl, q] = mn
        ls[sl, q] = ls[sl, q] * a + jnp.sum(w, axis=0, keepdims=True)
        acc[sl, q] = acc[sl, q] * a + jnp.dot(vt[sl, j], w.astype(BF), preferred_element_type=F32)

    inner = jnp.logical_or(c == 1, c == 2)

    def off_of(i):
        r = lax.rem(i, 4)
        far = jnp.where(inner, 5 - r, r)
        return jnp.where(r < 2, r, far)

    def seg_of(i):
        cc = c ^ off_of(i)
        low = (i < 4) == (y == 0)
        return jnp.where(low, cc, nseg - 1 - cc)

    def pos_of(s):
        low = s < 4
        off = jnp.where(low, s, nseg - 1 - s) ^ c
        far = jnp.where(inner, 5 - off, off)
        return jnp.where(low == (y == 0), 0, 4) + jnp.where(off < 2, off, far)

    def dest(s, hf):
        low = s < 4
        return jnp.where(low, s, nseg - 1 - s), jnp.where(low, hf, 2 + hf)

    def ocopy(sl, s, hf):
        c2, t2 = dest(s, hf)
        hd = t * 4 + 2 * sl + lax.rem(c, 2)
        src = ob.at[sl, s, pl.ds(hf * rows, rows)]
        dst = orecv.at[:, pl.ds(pl.multiple_of(hd * HD, HD), HD)]
        rm = remote(src, dst, osend.at[sl, s, hf], orsem.at[hd], c2, t2)
        lc = pltpu.make_async_copy(src, dst, orsem.at[hd])
        return jnp.logical_and(c2 == c, t2 == t), rm, lc

    def finish(sl, s):
        ob[sl, s] = (acc[sl, s] * (1.0 / ls[sl, s])).T.astype(BF)
        for hf in range(2):
            mine, rm, lc = ocopy(sl, s, hf)
            pl.when(jnp.logical_not(mine))(rm.start)
            pl.when(mine)(lc.start)

    def event(ev, _):
        p = ev // 8
        sl = lax.rem(ev // 4, 2)
        i = p * 4 + lax.rem(ev, 4)
        s = seg_of(i)
        off = off_of(i)
        for m in range(3):
            src, dst = blocks(m, p, c, sl, s)
            ok = need(m, c, sl, s)
            pl.when(jnp.logical_and(ok, off != 0))(
                remote(src, dst, bsend.at[0, 0, 0, 0], brecv.at[sl, m, s], c, t ^ 1).wait_recv)
            pl.when(jnp.logical_and(ok, off == 0))(
                pltpu.make_async_copy(src, dst, bloc.at[p, m, sl]).wait)

        def pair(k, _):
            s2 = seg_of(k)
            q, j = jnp.maximum(s, s2), jnp.minimum(s, s2)

            @pl.when(has(c, sl, q))
            def _():
                unit(sl, q, j, False)
            return 0

        lax.fori_loop(0, i, pair, 0)

        @pl.when(has(c, sl, s))
        def _():
            unit(sl, s, s, True)

        def done(q, last):
            last = jnp.maximum(last, pos_of(q))

            @pl.when(jnp.logical_and(last == i, has(c, sl, q)))
            def _():
                finish(sl, q)
            return last

        lax.fori_loop(0, nseg, done, 0)
        return 0

    lax.fori_loop(0, 16, event, 0)

    def wwait(tt):
        remote(wob.at[t], wob.at[tt], wsend.at[0], wrecv.at[tt], c, t ^ 1).wait_recv()

    wwait(t ^ 2)
    go(remote(wob.at[t ^ 2], wob.at[t ^ 2], wsend.at[2], wrecv.at[t ^ 2], c, t ^ 1))
    for i in range(1, 16):
        other = (c ^ (i // 4)) * 4 + (t ^ (i % 4))
        remote(cb, cnt.at[other], csend.at[i], crecv.at[other], c ^ (i // 4), t ^ (i % 4)).wait_recv()
    worst = jnp.max(cnt[...])
    over_ref[0] = (worst > BASE_CAP).astype(jnp.int32)
    for tt in range(4):
        for hd in range(4):
            k = tt * 4 + hd
            half_b = jnp.logical_and(seg0 >= 2, seg0 <= 5)
            if hd >= 2 and tt % 2 == 1:
                half_b = seg0 >= 2
            cp_ = jnp.where(half_b, 2, 0) + hd % 2
            mine = jnp.logical_and(cp_ == c, t == tt)
            dst = orecv.at[:, k * HD:(k + 1) * HD]
            src = ob.at[0, 0, pl.ds(0, rows)]
            pl.when(jnp.logical_not(mine))(remote(src, dst, osend.at[0, 0, 0], orsem.at[k], c, t ^ 1).wait_recv)
            pl.when(mine)(pltpu.make_async_copy(src, dst, orsem.at[k]).wait)
    wwait(t ^ 1)
    wwait(t ^ 3)
    for nb in range(4):
        cols = slice(nb * 512, (nb + 1) * 512)
        a = xs[own, cols].astype(F32)
        p = jnp.zeros_like(a)
        for tt in range(4):
            p = p + jnp.dot(orecv[:, tt * 512:(tt + 1) * 512], wob[tt, :, cols], preferred_element_type=F32)
        hs[:, cols] = (a + p).astype(BF)
    hcp = pltpu.make_async_copy(hs, h_out, hsem.at[0])
    hcp.start()
    experts(BASE_CAP, c, t, hs, it_ref[...], gt_ref[...], y_ref, wl, wg, wu, wd, sb, rb, zb, bb, *csems)
    hcp.wait()
    for cp in pending:
        cp.wait_send()
    for p, s in ((0, seg0), (1, seg1)):
        for m in range(3):
            for off in (1, 2, 3):
                for sl in range(2):
                    ok, cp = block_copy(m, p, off, sl, s)
                    pl.when(ok)(cp.wait_send)

    def drain(s, _):
        for sl in range(2):
            for hf in range(2):
                mine, rm, lc = ocopy(sl, s, hf)
                pl.when(jnp.logical_and(has(c, sl, s), jnp.logical_not(mine)))(rm.wait_send)
        return 0

    lax.fori_loop(0, nseg, drain, 0)


def experts(cap, c, t, h_ref, it, gt, y_ref, wl, wg, wu, wd, sb, rb, zb, bb, dsend, drecv, zsend, zrecv, dloc, zloc):
    me = c * 4 + t
    rows = h_ref.shape[0]
    ne = 16
    ei = lax.broadcasted_iota(jnp.int32, (HD, rows), 0)
    o0 = (it[0:1, :] == ei).astype(F32)
    o1 = (it[1:2, :] == ei).astype(F32)
    ri = lax.broadcasted_iota(jnp.int32, (rows, rows), 0)
    ci = lax.broadcasted_iota(jnp.int32, (rows, rows), 1)
    rank = jnp.dot((o0 + o1).astype(BF), (ri < ci).astype(BF), preferred_element_type=F32)
    base = jnp.where(rank < cap, ei.astype(F32) * cap + rank, -1.0)
    d0 = jnp.sum(o0 * base, axis=0, keepdims=True)
    d1 = jnp.sum(o1 * base, axis=0, keepdims=True)
    ki = lax.broadcasted_iota(jnp.int32, (ne * cap, rows), 0).astype(F32)
    pack = jnp.logical_or(ki == d0, ki == d1).astype(BF)
    sb[...] = jnp.dot(pack, h_ref[...], preferred_element_type=F32).astype(BF).reshape(sb.shape)
    sends = []
    for k in ORDER:
        off, i = k // 4, k % 4
        c2, t2 = c ^ off, t ^ i
        k2 = c2 * 4 + t2
        if k == 0:
            own = pltpu.make_async_copy(sb.at[me], rb.at[0], dloc.at[0])
            own.start()
        else:
            cp = remote(sb.at[k2], rb.at[k], dsend.at[k], drecv.at[k], c2, t2)
            cp.start()
            sends.append(cp)
    for cp in wl:
        cp.wait()
    for off in (0, 1, 2, 3):
        for i in range(4):
            k = off * 4 + i
            if k == 0:
                own.wait()
            else:
                remote(sb.at[0], rb.at[k], dsend.at[k], drecv.at[k], c ^ off, t ^ i).wait_recv()
        r = rb[off * 4:off * 4 + 4].reshape(4 * cap, -1)
        g = jnp.dot(r, wg[...], preferred_element_type=F32)
        u = jnp.dot(r, wu[...], preferred_element_type=F32)
        a = (g * jax.nn.sigmoid(g) * u).astype(BF)
        z = jnp.dot(a, wd[...], preferred_element_type=F32).astype(BF)
        zb[off * 4:off * 4 + 4] = z.reshape(4, cap, -1)
        for i in range(4):
            k = off * 4 + i
            if k == 0:
                zown = pltpu.make_async_copy(zb.at[0], bb.at[me], zloc.at[0])
                zown.start()
            else:
                cp = remote(zb.at[k], bb.at[me], zsend.at[k], zrecv.at[k], c ^ off, t ^ i)
                cp.start()
                sends.append(cp)
    cols8 = jnp.concatenate([d0, d1, gt, jnp.zeros((4, rows), F32)], axis=0).T
    kj = lax.broadcasted_iota(jnp.int32, (rows, ne * cap), 1).astype(F32)
    s0 = (kj == cols8[:, 0:1]).astype(BF)
    s1 = (kj == cols8[:, 1:2]).astype(BF)
    zown.wait()
    for k in range(1, 16):
        c2, t2 = c ^ (k // 4), t ^ (k % 4)
        remote(zb.at[0], bb.at[c2 * 4 + t2], zsend.at[k], zrecv.at[k], c2, t2).wait_recv()
    for nb in range(4):
        cols = slice(nb * 512, (nb + 1) * 512)
        b = bb[:, :, cols].reshape(ne * cap, 512)
        z0 = jnp.dot(s0, b, preferred_element_type=F32)
        z1 = jnp.dot(s1, b, preferred_element_type=F32)
        out = cols8[:, 2:3] * z0 + cols8[:, 3:4] * z1
        y_ref[:, cols] = (h_ref[:, cols].astype(F32) + out).astype(BF)
    for cp in sends:
        cp.wait_send()


def expert_loads(w1g_ref, w1u_ref, w2_ref, wg, wu, wd, wsem):
    return [pltpu.make_async_copy(a.at[0], b, wsem.at[i])
            for i, (a, b) in enumerate(((w1g_ref, wg), (w1u_ref, wu), (w2_ref, wd)))]


def kernel_c(cap, h_ref, it_ref, gt_ref, w1g_ref, w1u_ref, w2_ref, y_ref, wg, wu, wd, sb, rb, zb, bb, wsem, *sems):
    c = lax.axis_index('cp')
    t = lax.axis_index('tp')
    wl = expert_loads(w1g_ref, w1u_ref, w2_ref, wg, wu, wd, wsem)
    for cp in wl:
        cp.start()
    group_barrier(c, t)
    experts(cap, c, t, h_ref, it_ref[...], gt_ref[...], y_ref, wl, wg, wu, wd, sb, rb, zb, bb, *sems)


def params(cid):
    return pltpu.CompilerParams(collective_id=cid, has_side_effects=True, vmem_limit_bytes=63 * MIB)


def solution(mesh):
    rows_spec = P(('dp', 'cp', 'tp'), None)
    exp_spec = P(('cp', 'tp'), None, None)
    DMA = pltpu.SemaphoreType.DMA

    def local(x, idx, gates, wq, wk, wv, wo, w1g, w1u, w2):
        rows, d = x.shape
        seg = 2 * rows
        hc = wq.shape[1]
        ff = w1g.shape[2]
        sds = jax.ShapeDtypeStruct
        ew = [pltpu.VMEM((d, ff), BF), pltpu.VMEM((d, ff), BF), pltpu.VMEM((ff, d), BF)]
        es = [DMA((16,)), DMA((16,)), DMA((16,)), DMA((16,)), DMA((1,)), DMA((1,))]
        it, gt = idx.T, gates.T
        y, h, over = pl.pallas_call(
            kernel_ab, name='block',
            out_shape=(sds((rows, d), BF), sds((rows, d), BF), sds((1,), jnp.int32)),
            in_specs=[ANY, VM, VM] + [ANY] * 7, out_specs=(VM, ANY, pl.BlockSpec(memory_space=pltpu.SMEM)),
            scratch_shapes=[
                pltpu.VMEM((4 * rows, d), BF), pltpu.VMEM((d, hc), BF), pltpu.VMEM((d, hc), BF), pltpu.VMEM((d, hc), BF),
                pltpu.VMEM((2, 2, 4, seg, HD), BF), pltpu.VMEM((2, 4, HD, seg), BF),
                pltpu.VMEM((2, 2, 8, seg, HD), BF), pltpu.VMEM((2, 8, HD, seg), BF),
                pltpu.VMEM((2, 8, HD, seg), F32), pltpu.VMEM((2, 8, 1, seg), F32), pltpu.VMEM((2, 8, 1, seg), F32),
                pltpu.VMEM((4, hc, d), BF), pltpu.VMEM((2, 8, seg, HD), BF), pltpu.VMEM((rows, d), BF), pltpu.VMEM((rows, d), BF),
                pltpu.VMEM((8, HD), F32), pltpu.VMEM((16, 8, HD), F32)]
            + ew + [pltpu.VMEM((16, BASE_CAP, d), BF)] * 4
            + [DMA((5,)), DMA((3,)), DMA((4,)), DMA((3,)), DMA((4,)), DMA((2, 3, 4, 2)), DMA((2, 3, 8)), DMA((2, 3, 2)),
               DMA((2, 8, 2)), DMA((16,)), DMA((16,)), DMA((16,)), DMA((1,)), DMA((3,))] + es,
            compiler_params=params(0))(x, it, gt, wq, wk, wv, wo, w1g, w1u, w2)

        def full(h, y):
            return pl.pallas_call(
                functools.partial(kernel_c, FULL_CAP), name='experts_full',
                out_shape=sds((rows, d), BF),
                in_specs=[VM, VM, VM, ANY, ANY, ANY], out_specs=VM,
                scratch_shapes=ew + [pltpu.VMEM((16, FULL_CAP, d), BF)] * 4 + [DMA((3,))] + es,
                compiler_params=params(1))(h, it, gt, w1g, w1u, w2)

        return lax.cond(over[0] > 0, full, lambda h, y: y, h, y)

    return jax.shard_map(local, mesh=mesh, in_specs=(rows_spec, rows_spec, rows_spec, P(None, 'tp'), P(None, 'tp'), P(None, 'tp'), P('tp', None), exp_spec, exp_spec, exp_spec), out_specs=rows_spec, check_vma=False)
```

```python
import functools

import jax
import jax.numpy as jnp
from jax import lax
from jax.experimental import pallas as pl
from jax.experimental.pallas import tpu as pltpu
from jax.sharding import PartitionSpec as P

HD = 128
BF = jnp.bfloat16
F32 = jnp.float32
MESH = pl.DeviceIdType.MESH
NEG = -1e30
ANY = pl.BlockSpec(memory_space=pl.ANY)
VM = pl.BlockSpec(memory_space=pltpu.VMEM)
MIB = 2 ** 20
BASE_CAP, FULL_CAP = 32, 64
ORDER = (4, 5, 6, 7, 8, 9, 10, 11, 12, 13, 14, 15, 1, 2, 3, 0)


def remote(src, dst, ssem, rsem, c, t):
    return pltpu.make_async_remote_copy(
        src_ref=src, dst_ref=dst, send_sem=ssem, recv_sem=rsem,
        device_id={'cp': c, 'tp': t}, device_id_type=MESH)


def group_barrier(c, t, twin=None):
    sem = pltpu.get_barrier_semaphore()
    for i in range(1, 16):
        pl.semaphore_signal(sem, inc=1, device_id={'cp': c ^ (i // 4), 'tp': t ^ (i % 4)}, device_id_type=MESH)
    if twin is not None:
        pl.semaphore_signal(sem, inc=1, device_id={'dp': twin}, device_id_type=MESH)
    pl.semaphore_wait(sem, 15 if twin is None else 16)


def kernel_ab(x_ref, it_ref, gt_ref, wq_ref, wk_ref, wv_ref, wo_ref, w1g_ref, w1u_ref, w2_ref,
              y_ref, h_out, over_ref,
              xs, wq, wk, wv, sqk, sv, qk, vt, acc, mx, ls, wob, ob, orecv, hs, cb, cnt,
              wg, wu, wd, sb, rb, zb, bb,
              ldsem, xsend, xrecv, wsend, wrecv, bsend, brecv, bloc, osend, orsem, csend, crecv, hsem, esem, *csems):
    c = lax.axis_index('cp')
    t = lax.axis_index('tp')
    y = t // 2
    odd = lax.rem(t, 2) == 1
    rows = it_ref.shape[1]
    seg = 2 * rows
    nseg = 8
    me = c * 4 + t

    def pick(cc):
        return lax.rem(cc, 2)

    def moved(cc, sl):
        return jnp.logical_and(odd, sl == 1)

    def has(cc, sl, s):
        outer = jnp.logical_or(s < 2, s > 5)
        kept = jnp.where(cc < 2, outer, jnp.logical_not(outer))
        return jnp.where(moved(cc, sl), jnp.where(cc < 2, s < 2, s >= 2), kept)

    def sees(cc, sl, s):
        return s <= jnp.where(moved(cc, sl), jnp.where(cc < 2, 1, 7), jnp.where(cc < 2, 7, 5))

    own = pl.ds(pl.multiple_of(t * rows, rows), rows)
    loads = [pltpu.make_async_copy(a, b, ldsem.at[i])
             for i, (a, b) in enumerate(((x_ref, xs.at[own]), (wk_ref, wk), (wv_ref, wv), (wq_ref, wq), (wo_ref, wob.at[t])))]
    for cp in loads:
        cp.start()
    e = lax.broadcasted_iota(jnp.int32, (HD, rows), 0)
    hit = (it_ref[0:1, :] == e).astype(F32) + (it_ref[1:2, :] == e).astype(F32)
    load = jnp.max(jnp.sum(hit, axis=1, keepdims=True), axis=0, keepdims=True)
    cb[0] = jnp.broadcast_to(load, cb.shape[1:])
    twin = 1 - lax.axis_index('dp')
    group_barrier(c, t, twin)
    pending = []

    def go(cp):
        cp.start()
        pending.append(cp)

    tw = pltpu.make_async_remote_copy(
        src_ref=cb.at[0], dst_ref=cb.at[1], send_sem=csend.at[0], recv_sem=crecv.at[16],
        device_id={'dp': twin}, device_id_type=MESH)
    go(tw)
    loads[0].wait()
    go(remote(xs.at[own], xs.at[own], xsend.at[0], xrecv.at[t], c, t ^ 1))
    go(remote(xs.at[own], xs.at[own], xsend.at[1], xrecv.at[t], c, t ^ 2))

    def xwait(tt):
        r = pl.ds(pl.multiple_of(tt * rows, rows), rows)
        remote(xs.at[r], xs.at[r], xsend.at[0], xrecv.at[tt], c, t ^ 1).wait_recv()

    def blocks(m, p, cc, sl, s):
        hd = 2 * sl + pick(cc)
        if m == 2:
            return sv.at[p, hd], vt.at[sl, s]
        return sqk.at[p, m, hd], qk.at[sl, m, s]

    def need(m, cc, sl, s):
        return has(cc, sl, s) if m == 0 else sees(cc, sl, s)

    core = lax.rem(t, 2)

    def cut(m, ref, part):
        at = pl.ds(pl.multiple_of((core ^ part) * rows, rows), rows)
        return ref.at[:, at] if m == 2 else ref.at[at]

    def block_copy(m, p, off, sl, s, part):
        cc = c ^ off
        src, dst = blocks(m, p, cc, sl, s)
        return need(m, cc, sl, s), remote(cut(m, src, part), cut(m, dst, part), bsend.at[p, m, off, 2 * sl + part], brecv.at[sl, m, s], cc, t)

    def own_copy(m, p, sl, s):
        src, dst = blocks(m, p, c, sl, s)
        return need(m, c, sl, s), pltpu.make_async_copy(src, dst, bloc.at[p, m, sl])

    def half(p, tt, s, arrive):
        for sl in range(2):
            wide = slice(2 * sl * HD, 2 * (sl + 1) * HD)
            for part in range(2):
                if sl == 0:
                    arrive[part]()
                at = pl.ds(pl.multiple_of((core ^ part) * rows, rows), rows)
                xp = xs[pl.ds(pl.multiple_of((tt ^ part) * rows, rows), rows), :]
                for m, w, ld in ((1, wk, 1), (2, wv, 2), (0, wq, 3)):
                    if p == 0 and sl == 0 and part == 0:
                        loads[ld].wait()
                    r = jnp.dot(xp, w[:, wide], preferred_element_type=F32)
                    if m == 2:
                        rt = r.T.astype(BF)
                        for hh in range(2):
                            sv[p, 2 * sl + hh, :, at] = rt[hh * HD:(hh + 1) * HD]
                    else:
                        r = r.astype(BF)
                        for hh in range(2):
                            sqk[p, m, 2 * sl + hh, at] = r[:, hh * HD:(hh + 1) * HD]
                    for off in (1, 2, 3):
                        ok, cp = block_copy(m, p, off, sl, s, part)
                        pl.when(ok)(cp.start)
            for m in range(3):
                ok, cp = own_copy(m, p, sl, s)
                pl.when(ok)(cp.start)

    seg0 = jnp.where(y == 0, c, nseg - 1 - c)
    seg1 = jnp.where(y == 0, nseg - 1 - c, c)
    half(0, t, seg0, (lambda: None, lambda: xwait(t ^ 1)))
    loads[4].wait()
    go(remote(wob.at[t], wob.at[t], wsend.at[0], wrecv.at[t], c, t ^ 1))
    go(remote(wob.at[t], wob.at[t], wsend.at[1], wrecv.at[t], c, t ^ 2))
    tw.wait_recv()
    cb[2] = jnp.maximum(cb[0], cb[1])
    cnt[me] = cb[2]
    for i in range(1, 16):
        go(remote(cb.at[2], cnt.at[me], csend.at[i], crecv.at[me], c ^ (i // 4), t ^ (i % 4)))
    acc[...] = jnp.zeros_like(acc)
    mx[...] = jnp.full_like(mx, NEG)
    ls[...] = jnp.zeros_like(ls)
    def pass_on():
        xwait(t ^ 2)
        r2 = pl.ds(pl.multiple_of((t ^ 2) * rows, rows), rows)
        go(remote(xs.at[r2], xs.at[r2], xsend.at[2], xrecv.at[t ^ 2], c, t ^ 1))

    half(1, t ^ 2, seg1, (pass_on, lambda: xwait(t ^ 3)))
    wl = expert_loads(w1g_ref, w1u_ref, w2_ref, wg, wu, wd, esem)
    for cp in wl:
        cp.start()

    k2 = (HD ** -0.5) * 1.4426950408889634

    def unit(sl, q, j, diag):
        sc = lax.dot_general(qk[sl, 1, j], qk[sl, 0, q], (((1,), (1,)), ((), ())), preferred_element_type=F32)
        if diag:
            ki = lax.broadcasted_iota(jnp.int32, sc.shape, 0)
            qi = lax.broadcasted_iota(jnp.int32, sc.shape, 1)
            sc = jnp.where(ki <= qi, sc, NEG)
        m = mx[sl, q]
        mn = jnp.maximum(m, jnp.max(sc, axis=0, keepdims=True))
        w = jnp.exp2((sc - mn) * k2)
        a = jnp.exp2((m - mn) * k2)
        mx[sl, q] = mn
        ls[sl, q] = ls[sl, q] * a + jnp.sum(w, axis=0, keepdims=True)
        acc[sl, q] = acc[sl, q] * a + jnp.dot(vt[sl, j], w.astype(BF), preferred_element_type=F32)

    inner = jnp.logical_or(c == 1, c == 2)

    def off_of(i):
        r = lax.rem(i, 4)
        far = jnp.where(inner, 5 - r, r)
        return jnp.where(r < 2, r, far)

    def seg_of(i):
        cc = c ^ off_of(i)
        low = (i < 4) == (y == 0)
        return jnp.where(low, cc, nseg - 1 - cc)

    def pos_of(s):
        low = s < 4
        off = jnp.where(low, s, nseg - 1 - s) ^ c
        far = jnp.where(inner, 5 - off, off)
        return jnp.where(low == (y == 0), 0, 4) + jnp.where(off < 2, off, far)

    def dest(s, hf):
        low = s < 4
        return jnp.where(low, s, nseg - 1 - s), jnp.where(low, hf, 2 + hf)

    def ocopy(sl, s, hf):
        c2, t2 = dest(s, hf)
        hd = t * 4 + 2 * sl + pick(c)
        src = ob.at[sl, s, pl.ds(hf * rows, rows)]
        dst = orecv.at[:, pl.ds(pl.multiple_of(hd * HD, HD), HD)]
        rm = remote(src, dst, osend.at[sl, s, hf], orsem.at[hd], c2, t2)
        lc = pltpu.make_async_copy(src, dst, orsem.at[hd])
        return jnp.logical_and(c2 == c, t2 == t), rm, lc

    def finish(sl, s):
        ob[sl, s] = (acc[sl, s] * (1.0 / ls[sl, s])).T.astype(BF)
        for hf in range(2):
            mine, rm, lc = ocopy(sl, s, hf)
            pl.when(jnp.logical_not(mine))(rm.start)
            pl.when(mine)(lc.start)

    def event(ev, _):
        p = ev // 8
        sl = lax.rem(ev // 4, 2)
        i = p * 4 + lax.rem(ev, 4)
        s = seg_of(i)
        off = off_of(i)
        for m in range(3):
            src, dst = blocks(m, p, c, sl, s)
            ok = need(m, c, sl, s)
            pl.when(jnp.logical_and(ok, off != 0))(
                remote(src, dst, bsend.at[0, 0, 0, 0], brecv.at[sl, m, s], c, t ^ 1).wait_recv)
            pl.when(jnp.logical_and(ok, off == 0))(
                pltpu.make_async_copy(src, dst, bloc.at[p, m, sl]).wait)

        def pair(k, _):
            s2 = seg_of(k)
            q, j = jnp.maximum(s, s2), jnp.minimum(s, s2)

            @pl.when(has(c, sl, q))
            def _():
                unit(sl, q, j, False)
            return 0

        lax.fori_loop(0, i, pair, 0)

        @pl.when(has(c, sl, s))
        def _():
            unit(sl, s, s, True)

        def done(q, last):
            last = jnp.maximum(last, pos_of(q))

            @pl.when(jnp.logical_and(last == i, has(c, sl, q)))
            def _():
                finish(sl, q)
            return last

        lax.fori_loop(0, nseg, done, 0)
        return 0

    lax.fori_loop(0, 16, event, 0)

    def wwait(tt):
        remote(wob.at[t], wob.at[tt], wsend.at[0], wrecv.at[tt], c, t ^ 1).wait_recv()

    wwait(t ^ 2)
    go(remote(wob.at[t ^ 2], wob.at[t ^ 2], wsend.at[2], wrecv.at[t ^ 2], c, t ^ 1))
    for i in range(1, 16):
        other = (c ^ (i // 4)) * 4 + (t ^ (i % 4))
        remote(cb.at[2], cnt.at[other], csend.at[i], crecv.at[other], c ^ (i // 4), t ^ (i % 4)).wait_recv()
    worst = jnp.max(cnt[...])
    over_ref[0] = (worst > BASE_CAP).astype(jnp.int32)
    for tt in range(4):
        for hd in range(4):
            k = tt * 4 + hd
            half_b = jnp.logical_and(seg0 >= 2, seg0 <= 5)
            if tt % 2 == 1 and hd >= 2:
                half_b = seg0 >= 2
            cp_ = jnp.where(half_b, 2 + hd % 2, hd % 2)
            mine = jnp.logical_and(cp_ == c, t == tt)
            dst = orecv.at[:, k * HD:(k + 1) * HD]
            src = ob.at[0, 0, pl.ds(0, rows)]
            pl.when(jnp.logical_not(mine))(remote(src, dst, osend.at[0, 0, 0], orsem.at[k], c, t ^ 1).wait_recv)
            pl.when(mine)(pltpu.make_async_copy(src, dst, orsem.at[k]).wait)
    wwait(t ^ 1)
    wwait(t ^ 3)
    for nb in range(4):
        cols = slice(nb * 512, (nb + 1) * 512)
        a = xs[own, cols].astype(F32)
        p = jnp.zeros_like(a)
        for tt in range(4):
            p = p + jnp.dot(orecv[:, tt * 512:(tt + 1) * 512], wob[tt, :, cols], preferred_element_type=F32)
        hs[:, cols] = (a + p).astype(BF)
    hcp = pltpu.make_async_copy(hs, h_out, hsem.at[0])
    hcp.start()
    experts(BASE_CAP, c, t, hs, it_ref[...], gt_ref[...], y_ref, wl, wg, wu, wd, sb, rb, zb, bb, *csems)
    hcp.wait()
    for cp in pending:
        cp.wait_send()
    for p, s in ((0, seg0), (1, seg1)):
        for m in range(3):
            for off in (1, 2, 3):
                for sl in range(2):
                    for part in range(2):
                        ok, cp = block_copy(m, p, off, sl, s, part)
                        pl.when(ok)(cp.wait_send)

    def drain(s, _):
        for sl in range(2):
            for hf in range(2):
                mine, rm, lc = ocopy(sl, s, hf)
                pl.when(jnp.logical_and(has(c, sl, s), jnp.logical_not(mine)))(rm.wait_send)
        return 0

    lax.fori_loop(0, nseg, drain, 0)


def experts(cap, c, t, h_ref, it, gt, y_ref, wl, wg, wu, wd, sb, rb, zb, bb, dsend, drecv, zsend, zrecv, dloc, zloc):
    me = c * 4 + t
    rows = h_ref.shape[0]
    ne = 16
    ei = lax.broadcasted_iota(jnp.int32, (HD, rows), 0)
    o0 = (it[0:1, :] == ei).astype(F32)
    o1 = (it[1:2, :] == ei).astype(F32)
    ri = lax.broadcasted_iota(jnp.int32, (rows, rows), 0)
    ci = lax.broadcasted_iota(jnp.int32, (rows, rows), 1)
    rank = jnp.dot((o0 + o1).astype(BF), (ri < ci).astype(BF), preferred_element_type=F32)
    base = jnp.where(rank < cap, ei.astype(F32) * cap + rank, -1.0)
    d0 = jnp.sum(o0 * base, axis=0, keepdims=True)
    d1 = jnp.sum(o1 * base, axis=0, keepdims=True)
    ki = lax.broadcasted_iota(jnp.int32, (ne * cap, rows), 0).astype(F32)
    pack = jnp.logical_or(ki == d0, ki == d1).astype(BF)
    sb[...] = jnp.dot(pack, h_ref[...], preferred_element_type=F32).astype(BF).reshape(sb.shape)
    sends = []
    for k in ORDER:
        off, i = k // 4, k % 4
        c2, t2 = c ^ off, t ^ i
        k2 = c2 * 4 + t2
        if k == 0:
            own = pltpu.make_async_copy(sb.at[me], rb.at[0], dloc.at[0])
            own.start()
        else:
            cp = remote(sb.at[k2], rb.at[k], dsend.at[k], drecv.at[k], c2, t2)
            cp.start()
            sends.append(cp)
    for cp in wl:
        cp.wait()
    zown = pltpu.make_async_copy(zb.at[0], bb.at[me], zloc.at[0])

    def back(k):
        return remote(zb.at[k], bb.at[me], zsend.at[k], zrecv.at[k], c ^ (k // 4), t ^ lax.rem(k, 4))

    def group(off, _):
        for i in range(4):
            k = off * 4 + i
            arrived = remote(sb.at[0], rb.at[k], dsend.at[k], drecv.at[k], c ^ off, t ^ i).wait_recv
            if i == 0:
                pl.when(off == 0)(own.wait)
                pl.when(off > 0)(arrived)
            else:
                arrived()
        r = rb[pl.ds(off * 4, 4)].reshape(4 * cap, -1)
        g = jnp.dot(r, wg[...], preferred_element_type=F32)
        u = jnp.dot(r, wu[...], preferred_element_type=F32)
        a = (g * jax.nn.sigmoid(g) * u).astype(BF)
        z = jnp.dot(a, wd[...], preferred_element_type=F32).astype(BF)
        zb[pl.ds(off * 4, 4)] = z.reshape(4, cap, -1)
        for i in range(4):
            if i == 0:
                pl.when(off == 0)(zown.start)
                pl.when(off > 0)(back(off * 4).start)
            else:
                back(off * 4 + i).start()
        return 0

    lax.fori_loop(0, 4, group, 0)
    cols8 = jnp.concatenate([d0, d1, gt, jnp.zeros((4, rows), F32)], axis=0).T
    kj = lax.broadcasted_iota(jnp.int32, (rows, ne * cap), 1).astype(F32)
    s0 = (kj == cols8[:, 0:1]).astype(BF)
    s1 = (kj == cols8[:, 1:2]).astype(BF)
    zown.wait()
    for k in range(1, 16):
        c2, t2 = c ^ (k // 4), t ^ (k % 4)
        remote(zb.at[0], bb.at[c2 * 4 + t2], zsend.at[k], zrecv.at[k], c2, t2).wait_recv()
    for nb in range(4):
        cols = slice(nb * 512, (nb + 1) * 512)
        b = bb[:, :, cols].reshape(ne * cap, 512)
        z0 = jnp.dot(s0, b, preferred_element_type=F32)
        z1 = jnp.dot(s1, b, preferred_element_type=F32)
        out = cols8[:, 2:3] * z0 + cols8[:, 3:4] * z1
        y_ref[:, cols] = (h_ref[:, cols].astype(F32) + out).astype(BF)
    for cp in sends:
        cp.wait_send()
    for k in range(1, 16):
        back(k).wait_send()


def expert_loads(w1g_ref, w1u_ref, w2_ref, wg, wu, wd, wsem):
    return [pltpu.make_async_copy(a.at[0], b, wsem.at[i])
            for i, (a, b) in enumerate(((w1g_ref, wg), (w1u_ref, wu), (w2_ref, wd)))]


def kernel_c(cap, h_ref, it_ref, gt_ref, w1g_ref, w1u_ref, w2_ref, y_ref, wg, wu, wd, sb, rb, zb, bb, wsem, *sems):
    c = lax.axis_index('cp')
    t = lax.axis_index('tp')
    wl = expert_loads(w1g_ref, w1u_ref, w2_ref, wg, wu, wd, wsem)
    for cp in wl:
        cp.start()
    group_barrier(c, t)
    experts(cap, c, t, h_ref, it_ref[...], gt_ref[...], y_ref, wl, wg, wu, wd, sb, rb, zb, bb, *sems)


def params(cid):
    return pltpu.CompilerParams(collective_id=cid, has_side_effects=True, vmem_limit_bytes=60 * MIB)


def solution(mesh):
    rows_spec = P(('dp', 'cp', 'tp'), None)
    exp_spec = P(('cp', 'tp'), None, None)
    DMA = pltpu.SemaphoreType.DMA

    def local(x, idx, gates, wq, wk, wv, wo, w1g, w1u, w2):
        rows, d = x.shape
        seg = 2 * rows
        hc = wq.shape[1]
        ff = w1g.shape[2]
        sds = jax.ShapeDtypeStruct
        ew = [pltpu.VMEM((d, ff), BF), pltpu.VMEM((d, ff), BF), pltpu.VMEM((ff, d), BF)]
        es = [DMA((16,)), DMA((16,)), DMA((16,)), DMA((16,)), DMA((1,)), DMA((1,))]
        it, gt = idx.T, gates.T
        y, h, over = pl.pallas_call(
            kernel_ab, name='block',
            out_shape=(sds((rows, d), BF), sds((rows, d), BF), sds((1,), jnp.int32)),
            in_specs=[ANY, VM, VM] + [ANY] * 7, out_specs=(VM, ANY, pl.BlockSpec(memory_space=pltpu.SMEM)),
            scratch_shapes=[
                pltpu.VMEM((4 * rows, d), BF), pltpu.VMEM((d, hc), BF), pltpu.VMEM((d, hc), BF), pltpu.VMEM((d, hc), BF),
                pltpu.VMEM((2, 2, 4, seg, HD), BF), pltpu.VMEM((2, 4, HD, seg), BF),
                pltpu.VMEM((2, 2, 8, seg, HD), BF), pltpu.VMEM((2, 8, HD, seg), BF),
                pltpu.VMEM((2, 8, HD, seg), F32), pltpu.VMEM((2, 8, 1, seg), F32), pltpu.VMEM((2, 8, 1, seg), F32),
                pltpu.VMEM((4, hc, d), BF), pltpu.VMEM((2, 8, seg, HD), BF), pltpu.VMEM((rows, d), BF), pltpu.VMEM((rows, d), BF),
                pltpu.VMEM((3, 8, HD), F32), pltpu.VMEM((16, 8, HD), F32)]
            + ew + [pltpu.VMEM((16, BASE_CAP, d), BF)] * 4
            + [DMA((5,)), DMA((3,)), DMA((4,)), DMA((3,)), DMA((4,)), DMA((2, 3, 4, 4)), DMA((2, 3, 8)), DMA((2, 3, 2)),
               DMA((2, 8, 2)), DMA((16,)), DMA((16,)), DMA((17,)), DMA((1,)), DMA((3,))] + es,
            compiler_params=params(0))(x, it, gt, wq, wk, wv, wo, w1g, w1u, w2)

        def full(h, y):
            return pl.pallas_call(
                functools.partial(kernel_c, FULL_CAP), name='experts_full',
                out_shape=sds((rows, d), BF),
                in_specs=[VM, VM, VM, ANY, ANY, ANY], out_specs=VM,
                scratch_shapes=ew + [pltpu.VMEM((16, FULL_CAP, d), BF)] * 4 + [DMA((3,))] + es,
                compiler_params=params(1))(h, it, gt, w1g, w1u, w2)

        return lax.cond(over[0] > 0, full, lambda h, y: y, h, y)

    return jax.shard_map(local, mesh=mesh, in_specs=(rows_spec, rows_spec, rows_spec, P(None, 'tp'), P(None, 'tp'), P(None, 'tp'), P('tp', None), exp_spec, exp_spec, exp_spec), out_specs=rows_spec, check_vma=False)
```

```python
import functools

import jax
import jax.numpy as jnp
from jax import lax
from jax.experimental import pallas as pl
from jax.experimental.pallas import tpu as pltpu
from jax.sharding import PartitionSpec as P

HD = 128
BF = jnp.bfloat16
F32 = jnp.float32
MESH = pl.DeviceIdType.MESH
NEG = -1e30
ANY = pl.BlockSpec(memory_space=pl.ANY)
VM = pl.BlockSpec(memory_space=pltpu.VMEM)
MIB = 2 ** 20
BASE_CAP, FULL_CAP = 32, 64
ORDER = (4, 5, 6, 7, 8, 9, 10, 11, 12, 13, 14, 15, 1, 2, 3, 0)


def remote(src, dst, ssem, rsem, c, t):
    return pltpu.make_async_remote_copy(
        src_ref=src, dst_ref=dst, send_sem=ssem, recv_sem=rsem,
        device_id={'cp': c, 'tp': t}, device_id_type=MESH)


def group_barrier(c, t, twin=None):
    sem = pltpu.get_barrier_semaphore()
    for i in range(1, 16):
        pl.semaphore_signal(sem, inc=1, device_id={'cp': c ^ (i // 4), 'tp': t ^ (i % 4)}, device_id_type=MESH)
    if twin is not None:
        pl.semaphore_signal(sem, inc=1, device_id={'dp': twin}, device_id_type=MESH)
    pl.semaphore_wait(sem, 15 if twin is None else 16)


def kernel_ab(x_ref, it_ref, gt_ref, wq_ref, wk_ref, wv_ref, wo_ref, w1g_ref, w1u_ref, w2_ref,
              y_ref, h_out, over_ref,
              xs, wq, wk, wv, sqk, sv, qk, vt, acc, mx, ls, wob, ob, orecv, hs, cb, cnt,
              wg, wu, wd, sb, rb, zb, bb,
              ldsem, xsend, xrecv, wsend, wrecv, bsend, brecv, bloc, osend, orsem, csend, crecv, hsem, esem, *csems):
    c = lax.axis_index('cp')
    t = lax.axis_index('tp')
    y = t // 2
    odd = lax.rem(t, 2) == 1
    rows = it_ref.shape[1]
    seg = 2 * rows
    nseg = 8
    me = c * 4 + t

    def pick(cc):
        return lax.rem(cc, 2)

    def moved(cc, sl):
        return jnp.logical_and(odd, sl == 1)

    def has(cc, sl, s):
        outer = jnp.logical_or(s < 2, s > 5)
        kept = jnp.where(cc < 2, outer, jnp.logical_not(outer))
        return jnp.where(moved(cc, sl), jnp.where(cc < 2, s < 2, s >= 2), kept)

    def sees(cc, sl, s):
        return s <= jnp.where(moved(cc, sl), jnp.where(cc < 2, 1, 7), jnp.where(cc < 2, 7, 5))

    own = pl.ds(pl.multiple_of(t * rows, rows), rows)
    loads = [pltpu.make_async_copy(a, b, ldsem.at[i])
             for i, (a, b) in enumerate(((x_ref, xs.at[own]), (wk_ref, wk), (wv_ref, wv), (wq_ref, wq), (wo_ref, wob.at[t])))]
    for cp in loads:
        cp.start()
    e = lax.broadcasted_iota(jnp.int32, (HD, rows), 0)
    hit = (it_ref[0:1, :] == e).astype(F32) + (it_ref[1:2, :] == e).astype(F32)
    load = jnp.max(jnp.sum(hit, axis=1, keepdims=True), axis=0, keepdims=True)
    cb[0] = jnp.broadcast_to(load, cb.shape[1:])
    twin = 1 - lax.axis_index('dp')
    group_barrier(c, t, twin)
    pending = []

    def go(cp):
        cp.start()
        pending.append(cp)

    tw = pltpu.make_async_remote_copy(
        src_ref=cb.at[0], dst_ref=cb.at[1], send_sem=csend.at[0], recv_sem=crecv.at[16],
        device_id={'dp': twin}, device_id_type=MESH)
    go(tw)
    loads[0].wait()
    go(remote(xs.at[own], xs.at[own], xsend.at[0], xrecv.at[t], c, t ^ 1))
    go(remote(xs.at[own], xs.at[own], xsend.at[1], xrecv.at[t], c, t ^ 2))

    def xwait(tt):
        r = pl.ds(pl.multiple_of(tt * rows, rows), rows)
        remote(xs.at[r], xs.at[r], xsend.at[0], xrecv.at[tt], c, t ^ 1).wait_recv()

    def blocks(m, p, cc, sl, s):
        hd = 2 * sl + pick(cc)
        if m == 2:
            return sv.at[p, hd], vt.at[sl, s]
        return sqk.at[p, m, hd], qk.at[sl, m, s]

    def need(m, cc, sl, s):
        return has(cc, sl, s) if m == 0 else sees(cc, sl, s)

    core = lax.rem(t, 2)

    def cut(m, ref, part):
        at = pl.ds(pl.multiple_of((core ^ part) * rows, rows), rows)
        return ref.at[:, at] if m == 2 else ref.at[at]

    def block_copy(m, p, off, sl, s, part):
        cc = c ^ off
        src, dst = blocks(m, p, cc, sl, s)
        return need(m, cc, sl, s), remote(cut(m, src, part), cut(m, dst, part), bsend.at[p, m, off, 2 * sl + part], brecv.at[sl, m, s], cc, t)

    def own_copy(m, p, sl, s):
        src, dst = blocks(m, p, c, sl, s)
        return need(m, c, sl, s), pltpu.make_async_copy(src, dst, bloc.at[p, m, sl])

    def half(p, tt, s, arrive):
        for sl in range(2):
            wide = slice(2 * sl * HD, 2 * (sl + 1) * HD)
            for part in range(2):
                if sl == 0:
                    arrive[part]()
                at = pl.ds(pl.multiple_of((core ^ part) * rows, rows), rows)
                xp = xs[pl.ds(pl.multiple_of((tt ^ part) * rows, rows), rows), :]
                for m, w, ld in ((1, wk, 1), (2, wv, 2), (0, wq, 3)):
                    if p == 0 and sl == 0 and part == 0:
                        loads[ld].wait()
                    r = jnp.dot(xp, w[:, wide], preferred_element_type=F32)
                    if m == 2:
                        rt = r.T.astype(BF)
                        for hh in range(2):
                            sv[p, 2 * sl + hh, :, at] = rt[hh * HD:(hh + 1) * HD]
                    else:
                        r = r.astype(BF)
                        for hh in range(2):
                            sqk[p, m, 2 * sl + hh, at] = r[:, hh * HD:(hh + 1) * HD]
                    for off in (1, 2, 3):
                        ok, cp = block_copy(m, p, off, sl, s, part)
                        pl.when(ok)(cp.start)
            for m in range(3):
                ok, cp = own_copy(m, p, sl, s)
                pl.when(ok)(cp.start)

    seg0 = jnp.where(y == 0, c, nseg - 1 - c)
    seg1 = jnp.where(y == 0, nseg - 1 - c, c)
    half(0, t, seg0, (lambda: None, lambda: xwait(t ^ 1)))
    loads[4].wait()
    go(remote(wob.at[t], wob.at[t], wsend.at[0], wrecv.at[t], c, t ^ 1))
    go(remote(wob.at[t], wob.at[t], wsend.at[1], wrecv.at[t], c, t ^ 2))
    tw.wait_recv()
    cb[2] = jnp.maximum(cb[0], cb[1])
    cnt[me] = cb[2]
    for i in range(1, 16):
        go(remote(cb.at[2], cnt.at[me], csend.at[i], crecv.at[me], c ^ (i // 4), t ^ (i % 4)))
    acc[...] = jnp.zeros_like(acc)
    mx[...] = jnp.full_like(mx, NEG)
    ls[...] = jnp.zeros_like(ls)
    def pass_on():
        xwait(t ^ 2)
        r2 = pl.ds(pl.multiple_of((t ^ 2) * rows, rows), rows)
        go(remote(xs.at[r2], xs.at[r2], xsend.at[2], xrecv.at[t ^ 2], c, t ^ 1))

    half(1, t ^ 2, seg1, (pass_on, lambda: xwait(t ^ 3)))
    wl = expert_loads(w1g_ref, w1u_ref, w2_ref, wg, wu, wd, esem)
    for cp in wl:
        cp.start()

    k2 = (HD ** -0.5) * 1.4426950408889634

    def unit(sl, q, j, diag):
        sc = lax.dot_general(qk[sl, 1, j], qk[sl, 0, q], (((1,), (1,)), ((), ())), preferred_element_type=F32)
        if diag:
            ki = lax.broadcasted_iota(jnp.int32, sc.shape, 0)
            qi = lax.broadcasted_iota(jnp.int32, sc.shape, 1)
            sc = jnp.where(ki <= qi, sc, NEG)
        m = mx[sl, q]
        mn = jnp.maximum(m, jnp.max(sc, axis=0, keepdims=True))
        w = jnp.exp2((sc - mn) * k2)
        a = jnp.exp2((m - mn) * k2)
        mx[sl, q] = mn
        ls[sl, q] = ls[sl, q] * a + jnp.sum(w, axis=0, keepdims=True)
        acc[sl, q] = acc[sl, q] * a + jnp.dot(vt[sl, j], w.astype(BF), preferred_element_type=F32)

    inner = jnp.logical_or(c == 1, c == 2)

    def off_of(i):
        r = lax.rem(i, 4)
        far = jnp.where(inner, 5 - r, r)
        return jnp.where(r < 2, r, far)

    def seg_of(i):
        cc = c ^ off_of(i)
        low = (i < 4) == (y == 0)
        return jnp.where(low, cc, nseg - 1 - cc)

    def pos_of(s):
        low = s < 4
        off = jnp.where(low, s, nseg - 1 - s) ^ c
        far = jnp.where(inner, 5 - off, off)
        return jnp.where(low == (y == 0), 0, 4) + jnp.where(off < 2, off, far)

    def dest(s, hf):
        low = s < 4
        return jnp.where(low, s, nseg - 1 - s), jnp.where(low, hf, 2 + hf)

    def ocopy(sl, s, hf):
        c2, t2 = dest(s, hf)
        hd = t * 4 + 2 * sl + pick(c)
        src = ob.at[sl, s, pl.ds(hf * rows, rows)]
        dst = orecv.at[:, pl.ds(pl.multiple_of(hd * HD, HD), HD)]
        rm = remote(src, dst, osend.at[sl, s, hf], orsem.at[hd], c2, t2)
        lc = pltpu.make_async_copy(src, dst, orsem.at[hd])
        return jnp.logical_and(c2 == c, t2 == t), rm, lc

    def finish(sl, s):
        ob[sl, s] = (acc[sl, s] * (1.0 / ls[sl, s])).T.astype(BF)
        for hf in range(2):
            mine, rm, lc = ocopy(sl, s, hf)
            pl.when(jnp.logical_not(mine))(rm.start)
            pl.when(mine)(lc.start)

    def wwait(tt):
        remote(wob.at[t], wob.at[tt], wsend.at[0], wrecv.at[tt], c, t ^ 1).wait_recv()

    wpass = remote(wob.at[t ^ 2], wob.at[t ^ 2], wsend.at[2], wrecv.at[t ^ 2], c, t ^ 1)

    def event(ev, _):
        @pl.when(ev == 15)
        def _():
            wwait(t ^ 2)
            wpass.start()

        p = ev // 8
        sl = lax.rem(ev // 4, 2)
        i = p * 4 + lax.rem(ev, 4)
        s = seg_of(i)
        off = off_of(i)
        for m in range(3):
            src, dst = blocks(m, p, c, sl, s)
            ok = need(m, c, sl, s)
            pl.when(jnp.logical_and(ok, off != 0))(
                remote(src, dst, bsend.at[0, 0, 0, 0], brecv.at[sl, m, s], c, t ^ 1).wait_recv)
            pl.when(jnp.logical_and(ok, off == 0))(
                pltpu.make_async_copy(src, dst, bloc.at[p, m, sl]).wait)

        def pair(k, _):
            s2 = seg_of(k)
            q, j = jnp.maximum(s, s2), jnp.minimum(s, s2)

            @pl.when(has(c, sl, q))
            def _():
                unit(sl, q, j, False)
            return 0

        lax.fori_loop(0, i, pair, 0)

        @pl.when(has(c, sl, s))
        def _():
            unit(sl, s, s, True)

        def done(q, last):
            last = jnp.maximum(last, pos_of(q))

            @pl.when(jnp.logical_and(last == i, has(c, sl, q)))
            def _():
                finish(sl, q)
            return last

        lax.fori_loop(0, nseg, done, 0)
        return 0

    lax.fori_loop(0, 16, event, 0)
    pending.append(wpass)

    for i in range(1, 16):
        other = (c ^ (i // 4)) * 4 + (t ^ (i % 4))
        remote(cb.at[2], cnt.at[other], csend.at[i], crecv.at[other], c ^ (i // 4), t ^ (i % 4)).wait_recv()
    worst = jnp.max(cnt[...])
    over_ref[0] = (worst > BASE_CAP).astype(jnp.int32)
    def owait(tt, hd):
        k = tt * 4 + hd
        half_b = jnp.logical_and(seg0 >= 2, seg0 <= 5)
        if tt % 2 == 1 and hd >= 2:
            half_b = seg0 >= 2
        cp_ = jnp.where(half_b, 2 + hd % 2, hd % 2)
        mine = jnp.logical_and(cp_ == c, t == tt)
        dst = orecv.at[:, k * HD:(k + 1) * HD]
        src = ob.at[0, 0, pl.ds(0, rows)]
        pl.when(jnp.logical_not(mine))(remote(src, dst, osend.at[0, 0, 0], orsem.at[k], c, t ^ 1).wait_recv)
        pl.when(mine)(pltpu.make_async_copy(src, dst, orsem.at[k]).wait)

    wwait(t ^ 1)
    wwait(t ^ 3)
    for sl in range(2):
        for tt in range(4):
            for hd in (2 * sl, 2 * sl + 1):
                owait(tt, hd)
        ks = slice(2 * sl * HD, 2 * (sl + 1) * HD)
        for nb in range(4):
            cols = slice(nb * 512, (nb + 1) * 512)
            p = xs[own, cols].astype(F32) if sl else jnp.zeros((rows, 512), F32)
            q = acc[0, 2 * nb:2 * nb + 2].reshape(rows, 512) if sl else jnp.zeros((rows, 512), F32)
            for tt in range(4):
                o = orecv[:, tt * 512 + 2 * sl * HD:tt * 512 + 2 * (sl + 1) * HD]
                q = q + jnp.dot(o, wob[tt, ks, cols], preferred_element_type=F32)
            if sl:
                hs[:, cols] = (p + q).astype(BF)
            else:
                acc[0, 2 * nb:2 * nb + 2] = q.reshape(2, HD, 512)
    hcp = pltpu.make_async_copy(hs, h_out, hsem.at[0])
    hcp.start()
    experts(BASE_CAP, c, t, hs, it_ref[...], gt_ref[...], y_ref, wl, wg, wu, wd, sb, rb, zb, bb, *csems)
    hcp.wait()
    for cp in pending:
        cp.wait_send()
    for p, s in ((0, seg0), (1, seg1)):
        for m in range(3):
            for off in (1, 2, 3):
                for sl in range(2):
                    for part in range(2):
                        ok, cp = block_copy(m, p, off, sl, s, part)
                        pl.when(ok)(cp.wait_send)

    def drain(s, _):
        for sl in range(2):
            for hf in range(2):
                mine, rm, lc = ocopy(sl, s, hf)
                pl.when(jnp.logical_and(has(c, sl, s), jnp.logical_not(mine)))(rm.wait_send)
        return 0

    lax.fori_loop(0, nseg, drain, 0)


def experts(cap, c, t, h_ref, it, gt, y_ref, wl, wg, wu, wd, sb, rb, zb, bb, dsend, drecv, zsend, zrecv, dloc, zloc):
    me = c * 4 + t
    rows = h_ref.shape[0]
    ne = 16
    ei = lax.broadcasted_iota(jnp.int32, (HD, rows), 0)
    o0 = (it[0:1, :] == ei).astype(F32)
    o1 = (it[1:2, :] == ei).astype(F32)
    ri = lax.broadcasted_iota(jnp.int32, (rows, rows), 0)
    ci = lax.broadcasted_iota(jnp.int32, (rows, rows), 1)
    rank = jnp.dot((o0 + o1).astype(BF), (ri < ci).astype(BF), preferred_element_type=F32)
    base = jnp.where(rank < cap, ei.astype(F32) * cap + rank, -1.0)
    d0 = jnp.sum(o0 * base, axis=0, keepdims=True)
    d1 = jnp.sum(o1 * base, axis=0, keepdims=True)
    ki = lax.broadcasted_iota(jnp.int32, (ne * cap, rows), 0).astype(F32)
    pack = jnp.logical_or(ki == d0, ki == d1).astype(BF)
    sb[...] = jnp.dot(pack, h_ref[...], preferred_element_type=F32).astype(BF).reshape(sb.shape)
    sends = []
    for k in ORDER:
        off, i = k // 4, k % 4
        c2, t2 = c ^ off, t ^ i
        k2 = c2 * 4 + t2
        if k == 0:
            own = pltpu.make_async_copy(sb.at[me], rb.at[0], dloc.at[0])
            own.start()
        else:
            cp = remote(sb.at[k2], rb.at[k], dsend.at[k], drecv.at[k], c2, t2)
            cp.start()
            sends.append(cp)
    for cp in wl:
        cp.wait()
    zown = pltpu.make_async_copy(zb.at[0], bb.at[me], zloc.at[0])

    def back(k):
        return remote(zb.at[k], bb.at[me], zsend.at[k], zrecv.at[k], c ^ (k // 4), t ^ lax.rem(k, 4))

    def group(off, _):
        for i in range(4):
            k = off * 4 + i
            arrived = remote(sb.at[0], rb.at[k], dsend.at[k], drecv.at[k], c ^ off, t ^ i).wait_recv
            if i == 0:
                pl.when(off == 0)(own.wait)
                pl.when(off > 0)(arrived)
            else:
                arrived()
        r = rb[pl.ds(off * 4, 4)].reshape(4 * cap, -1)
        g = jnp.dot(r, wg[...], preferred_element_type=F32)
        u = jnp.dot(r, wu[...], preferred_element_type=F32)
        a = (g * jax.nn.sigmoid(g) * u).astype(BF)
        z = jnp.dot(a, wd[...], preferred_element_type=F32).astype(BF)
        zb[pl.ds(off * 4, 4)] = z.reshape(4, cap, -1)
        for i in range(4):
            if i == 0:
                pl.when(off == 0)(zown.start)
                pl.when(off > 0)(back(off * 4).start)
            else:
                back(off * 4 + i).start()
        return 0

    lax.fori_loop(0, 4, group, 0)
    cols8 = jnp.concatenate([d0, d1, gt, jnp.zeros((4, rows), F32)], axis=0).T
    kj = lax.broadcasted_iota(jnp.int32, (rows, ne * cap), 1).astype(F32)
    s0 = (kj == cols8[:, 0:1]).astype(BF)
    s1 = (kj == cols8[:, 1:2]).astype(BF)
    zown.wait()
    for k in range(1, 16):
        c2, t2 = c ^ (k // 4), t ^ (k % 4)
        remote(zb.at[0], bb.at[c2 * 4 + t2], zsend.at[k], zrecv.at[k], c2, t2).wait_recv()
    for nb in range(4):
        cols = slice(nb * 512, (nb + 1) * 512)
        b = bb[:, :, cols].reshape(ne * cap, 512)
        z0 = jnp.dot(s0, b, preferred_element_type=F32)
        z1 = jnp.dot(s1, b, preferred_element_type=F32)
        out = cols8[:, 2:3] * z0 + cols8[:, 3:4] * z1
        y_ref[:, cols] = (h_ref[:, cols].astype(F32) + out).astype(BF)
    for cp in sends:
        cp.wait_send()
    for k in range(1, 16):
        back(k).wait_send()


def expert_loads(w1g_ref, w1u_ref, w2_ref, wg, wu, wd, wsem):
    return [pltpu.make_async_copy(a.at[0], b, wsem.at[i])
            for i, (a, b) in enumerate(((w1g_ref, wg), (w1u_ref, wu), (w2_ref, wd)))]


def kernel_c(cap, h_ref, it_ref, gt_ref, w1g_ref, w1u_ref, w2_ref, y_ref, wg, wu, wd, sb, rb, zb, bb, wsem, *sems):
    c = lax.axis_index('cp')
    t = lax.axis_index('tp')
    wl = expert_loads(w1g_ref, w1u_ref, w2_ref, wg, wu, wd, wsem)
    for cp in wl:
        cp.start()
    group_barrier(c, t)
    experts(cap, c, t, h_ref, it_ref[...], gt_ref[...], y_ref, wl, wg, wu, wd, sb, rb, zb, bb, *sems)


def params(cid):
    return pltpu.CompilerParams(collective_id=cid, has_side_effects=True, vmem_limit_bytes=60 * MIB)


def solution(mesh):
    rows_spec = P(('dp', 'cp', 'tp'), None)
    exp_spec = P(('cp', 'tp'), None, None)
    DMA = pltpu.SemaphoreType.DMA

    def local(x, idx, gates, wq, wk, wv, wo, w1g, w1u, w2):
        rows, d = x.shape
        seg = 2 * rows
        hc = wq.shape[1]
        ff = w1g.shape[2]
        sds = jax.ShapeDtypeStruct
        ew = [pltpu.VMEM((d, ff), BF), pltpu.VMEM((d, ff), BF), pltpu.VMEM((ff, d), BF)]
        es = [DMA((16,)), DMA((16,)), DMA((16,)), DMA((16,)), DMA((1,)), DMA((1,))]
        it, gt = idx.T, gates.T
        y, h, over = pl.pallas_call(
            kernel_ab, name='block',
            out_shape=(sds((rows, d), BF), sds((rows, d), BF), sds((1,), jnp.int32)),
            in_specs=[ANY, VM, VM] + [ANY] * 7, out_specs=(VM, ANY, pl.BlockSpec(memory_space=pltpu.SMEM)),
            scratch_shapes=[
                pltpu.VMEM((4 * rows, d), BF), pltpu.VMEM((d, hc), BF), pltpu.VMEM((d, hc), BF), pltpu.VMEM((d, hc), BF),
                pltpu.VMEM((2, 2, 4, seg, HD), BF), pltpu.VMEM((2, 4, HD, seg), BF),
                pltpu.VMEM((2, 2, 8, seg, HD), BF), pltpu.VMEM((2, 8, HD, seg), BF),
                pltpu.VMEM((2, 8, HD, seg), F32), pltpu.VMEM((2, 8, 1, seg), F32), pltpu.VMEM((2, 8, 1, seg), F32),
                pltpu.VMEM((4, hc, d), BF), pltpu.VMEM((2, 8, seg, HD), BF), pltpu.VMEM((rows, d), BF), pltpu.VMEM((rows, d), BF),
                pltpu.VMEM((3, 8, HD), F32), pltpu.VMEM((16, 8, HD), F32)]
            + ew + [pltpu.VMEM((16, BASE_CAP, d), BF)] * 4
            + [DMA((5,)), DMA((3,)), DMA((4,)), DMA((3,)), DMA((4,)), DMA((2, 3, 4, 4)), DMA((2, 3, 8)), DMA((2, 3, 2)),
               DMA((2, 8, 2)), DMA((16,)), DMA((16,)), DMA((17,)), DMA((1,)), DMA((3,))] + es,
            compiler_params=params(0))(x, it, gt, wq, wk, wv, wo, w1g, w1u, w2)

        def full(h, y):
            return pl.pallas_call(
                functools.partial(kernel_c, FULL_CAP), name='experts_full',
                out_shape=sds((rows, d), BF),
                in_specs=[VM, VM, VM, ANY, ANY, ANY], out_specs=VM,
                scratch_shapes=ew + [pltpu.VMEM((16, FULL_CAP, d), BF)] * 4 + [DMA((3,))] + es,
                compiler_params=params(1))(h, it, gt, w1g, w1u, w2)

        return lax.cond(over[0] > 0, full, lambda h, y: y, h, y)

    return jax.shard_map(local, mesh=mesh, in_specs=(rows_spec, rows_spec, rows_spec, P(None, 'tp'), P(None, 'tp'), P(None, 'tp'), P('tp', None), exp_spec, exp_spec, exp_spec), out_specs=rows_spec, check_vma=False)
```
